256 devices in a mesh: batch: 4 (over y_lo, core), seq: 16 (over y_hi, z), heads: 4 (over x).
Axes of the slice: x: 4, y: 4 (y_hi: 2, y_lo: 2; y = y_hi * 2 + y_lo), z: 8, core: 2. Of those that a mesh axis runs over, the one named last changes fastest.
Arguments:
- hidden_in: bfloat16 [48, 5120], P('batch', 'seq'), may hold values from -7 to 7
- lengths: int32 [48], P('batch'), may hold values from 1 to 4096
- draft_ids: int32 [48], P('batch'), may hold values from 0 to 31999
- input_gain: float32 [5120], P('seq'), may hold values from 0.5 to 1.5
- w_query: bfloat16 [5120, 5120], P('seq', 'heads'), may hold values from -0.078125 to 0.078125
- w_latent: bfloat16 [5120, 4, 640], P('seq', 'heads'), may hold values from -0.078125 to 0.078125
- latent_cache: bfloat16 [48, 4, 4096, 640], P('batch', 'heads', 'seq'), may hold values from -1200 to 1200
- key_up: bfloat16 [4, 320, 1280], P('heads'), may hold values from -0.3125 to 0.3125
- value_up: bfloat16 [4, 320, 1280], P('heads'), may hold values from -0.3125 to 0.3125
- w_out: bfloat16 [5120, 5120], P('heads', 'seq'), may hold values from -0.078125 to 0.078125
- final_gain: float32 [5120], P('seq'), may hold values from 0.1 to 1.9
- w_vocab: bfloat16 [5120, 32000], P('seq', 'heads'), may hold values from -0.26 to 0.26
Outputs:
- new_hidden: bfloat16 [48, 5120], P('batch', 'seq')
- log_probs: float32 [48, 32000], P('batch', 'heads')
- draft_logprob: float32 [48], P('batch')
The draws below stay inside these ranges and needn't reach their ends.
Inputs may be any that keep to these rules, and one draw needn't show every extreme that they name: `lengths`: cache positions below a request's length are its live context.
All inputs are finite; a program needn't handle non-finite values.
Results may differ from the reference program's by a relative error of at most 0.012.
The reference program's roundings to bfloat16 on the way count: a program that leaves them out, or rounds other values in their place, can miss the bound.
Values sent between devices are 32-bit elements; how exact they have to be, the bound alone decides.
A program may use at most 64 MiB of HBM per device.

```python
import math
import jax
import jax.numpy as jnp
from jax import lax

D = 5120
HEADS = 40
HEAD_DIM = 128
VOCAB = 32000
GROUP_HEADS = 10
GROUP_RANK = 320
BATCH = 48
CONTEXT = 4096
GROUPS = 4


planted_pairs = 4


def hidden_rows(key):
    value_key = jax.random.fold_in(jax.random.fold_in(key, 11), 0)
    return jnp.clip(jax.random.normal(value_key, (BATCH, D), jnp.float32), -6.0, 6.0)


def draw_hidden_in(key, part):
    return hidden_rows(key).astype(jnp.bfloat16)


def draw_w_vocab(key, part):
    subkeys = jax.random.split(jax.random.fold_in(key, 23), 1)
    base = jnp.clip(jax.random.normal(subkeys[0], (D, VOCAB), jnp.float32), -6.0, 6.0)
    rising = jnp.exp(jnp.linspace(0.0, math.log(2.5), VOCAB, dtype=jnp.float32))
    table = base * float(D) ** (-0.5) * rising[None, :]
    return table.astype(jnp.bfloat16)


def drawn_spots(subkey):
    return jax.random.permutation(subkey, CONTEXT)[:2 * planted_pairs]


def planted_table(key):
    subkeys = jax.random.split(key, 6)
    shape = (BATCH, CONTEXT, 2 * GROUP_RANK)
    table = jnp.clip(jax.random.normal(subkeys[0], shape, jnp.float32), -6.0, 6.0)
    chosen = jax.random.bernoulli(subkeys[1], 0.4, (BATCH,))
    spots = jax.vmap(drawn_spots)(jax.random.split(subkeys[2], BATCH))
    strength = jnp.exp(jax.random.uniform(subkeys[3], (BATCH, planted_pairs, 1), jnp.float32, math.log(120.0), math.log(300.0)))
    direction = jnp.clip(jax.random.normal(subkeys[4], (BATCH, planted_pairs, GROUP_RANK), jnp.float32), -4.0, 4.0)
    shrink = jax.random.uniform(subkeys[5], (BATCH, planted_pairs, 1), jnp.float32, 0.005, 0.01)
    first_keys = strength * direction
    second_keys = first_keys * (1.0 - shrink)
    planted = jnp.concatenate([first_keys, second_keys], axis=1)
    request_index = jnp.arange(BATCH, dtype=jnp.int32)[:, None]
    current = table[request_index, spots, :GROUP_RANK]
    table = table.at[request_index, spots, :GROUP_RANK].set(jnp.where(chosen[:, None, None], planted, current))
    return table


def draw_latent_cache(key, part):
    groups_list = [planted_table(jax.random.fold_in(key, 101 + index)).astype(jnp.bfloat16) for index in range(GROUPS)]
    return jnp.stack(groups_list, axis=1)


def place_ends(values, rng, smallest, high):
    spot = [jax.random.randint(jax.random.fold_in(rng, axis), (), 0, length) for axis, length in enumerate(values.shape)]
    widest = values.shape.index(max(values.shape))
    beside = spot[:widest] + [(spot[widest] + 1) % values.shape[widest]] + spot[widest + 1:]
    return values.at[tuple(spot)].set(smallest).at[tuple(beside)].set(high)


def shard_levels(stream_key, dims, cuts, least, largest):
    loudness, own = 1.0, jax.random.fold_in(stream_key, 6)
    for axis_at, shards_of in cuts:
        heights = jnp.exp(jax.random.uniform(jax.random.fold_in(own, axis_at), (shards_of,), jnp.float32, least / len(cuts), largest / len(cuts)))
        loudness = loudness * jnp.repeat(heights, dims[axis_at] // shards_of).reshape([-1 if axis == axis_at else 1 for axis in range(len(dims))])
    return loudness


def bell_draw(key, extent, deviation, limit, cuts=(), held_as=jnp.bfloat16):
    result = jax.random.normal(key, extent, jnp.float32) * deviation
    if len(cuts) > 0:
        result = shard_levels(key, extent, cuts, -0.22, 0.18) * result
    return jnp.clip(result, min=-limit, max=limit).astype(held_as)


def setup_inputs(seed: int = 0) -> dict:
    streams_of = jax.random.split(jax.random.key(seed), 13)
    hidden_in = draw_hidden_in(jax.random.fold_in(streams_of[12], 71), 0)
    lengths = place_ends(jax.random.randint(streams_of[1], (BATCH,), 1, CONTEXT + 1), jax.random.fold_in(streams_of[1], 1), 1, CONTEXT).astype(jnp.int32)
    draft_ids = place_ends(jax.random.randint(streams_of[2], (BATCH,), 0, VOCAB), jax.random.fold_in(streams_of[2], 1), 0, VOCAB - 1).astype(jnp.int32)
    input_gain = jnp.clip(1.0 + 0.1 * jax.random.normal(streams_of[3], (D,), jnp.float32), 0.5, 1.5)
    w_query = bell_draw(streams_of[4], (D, HEADS * HEAD_DIM), D ** -0.5, 0.078125, ((0, 16), (1, 4)))
    w_latent = bell_draw(streams_of[5], (D, GROUPS, 2 * GROUP_RANK), D ** -0.5, 0.078125, ((0, 16), (1, 4)))
    latent_cache = draw_latent_cache(jax.random.fold_in(streams_of[12], 71), 0)
    key_up = bell_draw(streams_of[7], (GROUPS, GROUP_RANK, GROUP_HEADS * HEAD_DIM), GROUP_RANK ** -0.5, 0.3125, ((0, 4),))
    value_up = bell_draw(streams_of[8], (GROUPS, GROUP_RANK, GROUP_HEADS * HEAD_DIM), GROUP_RANK ** -0.5, 0.3125, ((0, 4),))
    w_out = bell_draw(streams_of[9], (HEADS * HEAD_DIM, D), (HEADS * HEAD_DIM) ** -0.5, 0.078125, ((0, 4), (1, 16)))
    final_gain = jnp.clip(1.0 + 0.18 * jax.random.normal(streams_of[10], (D,), jnp.float32), 0.1, 1.9)
    w_vocab = draw_w_vocab(jax.random.fold_in(streams_of[12], 71), 0)
    return {"hidden_in": hidden_in, "lengths": lengths, "draft_ids": draft_ids, "input_gain": input_gain, "w_query": w_query, "w_latent": w_latent, "latent_cache": latent_cache, "key_up": key_up, "value_up": value_up, "w_out": w_out, "final_gain": final_gain, "w_vocab": w_vocab}


epsilon = 1e-05
negative_fill = -1e+30

def attend_group(query_group, latent_group, cache_slab, key_map, value_map, lengths):
    batch_rows = query_group.shape[0]
    scaling = 1.0 / math.sqrt(HEAD_DIM)
    highest_prec = lax.Precision.HIGHEST
    heads_query = query_group.reshape(batch_rows, GROUP_HEADS, HEAD_DIM).astype(jnp.float32)
    key_table = key_map.astype(jnp.float32).reshape(GROUP_RANK, GROUP_HEADS, HEAD_DIM)
    absorbed_low = jnp.einsum('bhd,rhd->bhr', heads_query, key_table, precision=highest_prec).astype(jnp.bfloat16)
    absorbed = lax.optimization_barrier(absorbed_low).astype(jnp.float32)
    key_rows = cache_slab[:, :, :GROUP_RANK].astype(jnp.float32)
    value_rows = cache_slab[:, :, GROUP_RANK:].astype(jnp.float32)
    scores = jnp.einsum('bhr,btr->bht', absorbed, key_rows, precision=highest_prec) * scaling
    positions = jnp.arange(CONTEXT, dtype=jnp.int32)
    live_mask = positions[None, None, :] < lengths[:, None, None]
    scores = jnp.where(live_mask, scores, negative_fill)
    own_key = latent_group[:, :GROUP_RANK].astype(jnp.float32)
    own_value = latent_group[:, GROUP_RANK:].astype(jnp.float32)
    own_score = jnp.einsum('bhr,br->bh', absorbed, own_key, precision=highest_prec) * scaling
    highest = jnp.maximum(lax.optimization_barrier(jnp.max(scores, axis=2)), own_score)
    weights = jnp.where(live_mask, jnp.exp(scores - highest[..., None]), 0.0)
    own_weight = jnp.exp(own_score - highest)
    denominator = lax.optimization_barrier(jnp.sum(weights, axis=2)) + own_weight
    rounded = lax.optimization_barrier(weights.astype(jnp.bfloat16)).astype(jnp.float32)
    mixed_sum = jnp.einsum('bht,btr->bhr', rounded, value_rows, precision=highest_prec)
    mixed_sum = mixed_sum + own_weight[..., None] * own_value[:, None, :]
    latent_out = mixed_sum / denominator[..., None]
    value_table = value_map.astype(jnp.float32).reshape(GROUP_RANK, GROUP_HEADS, HEAD_DIM)
    head_out = jnp.einsum('bhr,rhd->bhd', latent_out, value_table, precision=highest_prec).astype(jnp.bfloat16)
    return head_out.reshape(batch_rows, GROUP_HEADS * HEAD_DIM)

def reference(hidden_in, lengths, draft_ids, input_gain, w_query, w_latent, latent_cache, key_up, value_up, w_out, final_gain, w_vocab):
    states = hidden_in.astype(jnp.float32)
    inv_rms = lax.rsqrt(lax.optimization_barrier(jnp.mean(states * states, axis=1, keepdims=True)) + epsilon)
    gained = (states * input_gain).astype(jnp.bfloat16)
    query_rows = (inv_rms * jnp.dot(gained, w_query, preferred_element_type=jnp.float32)).astype(jnp.bfloat16)
    latent_matrix = w_latent.reshape(D, GROUPS * 2 * GROUP_RANK)
    latent = (inv_rms * jnp.dot(gained, latent_matrix, preferred_element_type=jnp.float32)).astype(jnp.bfloat16)
    head_width = GROUP_HEADS * HEAD_DIM
    latent_width = 2 * GROUP_RANK
    pieces = []
    for group_idx in range(GROUPS):
        pieces.append(attend_group(query_rows[:, group_idx * head_width:(group_idx + 1) * head_width], latent[:, group_idx * latent_width:(group_idx + 1) * latent_width], latent_cache[:, group_idx], key_up[group_idx], value_up[group_idx], lengths))
    heads_out = jnp.concatenate(pieces, axis=1)
    updated = states + jnp.dot(heads_out, w_out, preferred_element_type=jnp.float32)
    new_hidden = updated.astype(jnp.bfloat16)
    inv_final = lax.rsqrt(lax.optimization_barrier(jnp.mean(updated * updated, axis=1, keepdims=True)) + epsilon)
    final_scaled = (updated * final_gain).astype(jnp.bfloat16)
    logits = inv_final * jnp.dot(final_scaled, w_vocab, preferred_element_type=jnp.float32)
    highest = lax.optimization_barrier(jnp.max(logits, axis=1, keepdims=True))
    log_total = highest + jnp.log(lax.optimization_barrier(jnp.sum(jnp.exp(logits - highest), axis=1, keepdims=True)))
    log_probs = logits - log_total
    picked = jnp.take_along_axis(logits, draft_ids[:, None].astype(jnp.int32), axis=1)[:, 0]
    draft_logprob = picked - log_total[:, 0]
    return (new_hidden, log_probs, draft_logprob)
```

```python
import functools
import math

import jax
import jax.numpy as jnp
from jax import lax
from jax.experimental import pallas as pl
from jax.experimental.pallas import tpu as pltpu
from jax.sharding import PartitionSpec as P

D = 5120
HEAD_DIM = 128
GROUP_HEADS = 10
RANK = 320
SEQ = 16
ROWS = 12
SPAN = 256
WIDE = 512
VOCAB_LOCAL = 8000
PIECES = 15
TAIL = VOCAB_LOCAL - 15 * WIDE

MESH = pl.DeviceIdType.MESH
f32 = jnp.float32
bf16 = jnp.bfloat16
epsilon = 1e-05
negative_fill = -1e30
scaling = 1.0 / math.sqrt(HEAD_DIM)

QUERY_SUM, QUERY_ALL, HEAD_SUM, HEAD_ALL, SQUARES, VOCAB_SUM, VOCAB_ALL = range(7)


def owner_of_head(k):
    return lax.div(k * 8, 5)


def head_of_owner(s):
    return lax.div(s * 5 + 7, 8)


def owns_head(s):
    return owner_of_head(head_of_owner(s)) == s


def iota(shape, dim):
    return lax.broadcasted_iota(jnp.int32, shape, dim)


def as_row(column):
    spread = jnp.where(iota((16, 128), 0) == iota((16, 128), 1), column, 0.0)
    return jnp.sum(spread, axis=0, keepdims=True)


def as_column(row, picks):
    return jnp.sum(jnp.where(picks == iota(picks.shape, 1), row, 0.0), axis=1, keepdims=True)


def kernel(
    heads_size,
    hidden, lengths, drafts, gain, wq, wl, cache, ku, vu, wo, fgain, wv,
    new_hidden, log_probs, draft_out,
    hid_v, len_s, draft_s, gain_v, wq_v, wl_v, cache_v, ku_v, vu_v, wo_v, fgain_v, wv_v,
    states_v,
    qa_send, qa_recv, qa_all,
    absorbed_v, mixed_v,
    hb_send, hb_recv, hb_all, own_v,
    at_send, at_recv,
    sq_send, sq_recv,
    vd_send, vd_recv, vd_all,
    st_send, st_recv,
    load_sem, send_sem, recv_sem, x_send_sem, x_recv_sem,
):
    me = lax.axis_index("seq")
    hme = lax.axis_index("heads")

    loads = [
        (hidden, hid_v), (gain, gain_v), (lengths, len_s), (drafts, draft_s), (fgain, fgain_v),
        (wq, wq_v), (wl, wl_v), (ku, ku_v), (cache, cache_v), (vu, vu_v.at[pl.ds(64, RANK)]),
        (wo, wo_v), (wv, wv_v),
    ]
    loads = [pltpu.make_async_copy(a, b, load_sem.at[i]) for i, (a, b) in enumerate(loads)]
    l_hid, l_gain, l_len, l_draft, l_fgain, l_wq, l_wl, l_ku, l_cache, l_vu, l_wo, l_wv = loads
    for load in loads:
        load.start()

    barrier = pltpu.get_barrier_semaphore()

    @pl.loop(1, SEQ)
    def _(j):
        pl.semaphore_signal(
            barrier, inc=1, device_id={"seq": lax.rem(me + j, SEQ)}, device_id_type=MESH
        )

    for j in range(1, heads_size):
        pl.semaphore_signal(
            barrier, inc=1, device_id={"heads": lax.rem(hme + j, heads_size)}, device_id_type=MESH
        )

    def over_seq(phase, src, dst, peer):
        return pltpu.make_async_remote_copy(
            src_ref=src, dst_ref=dst,
            send_sem=send_sem.at[phase, peer], recv_sem=recv_sem.at[phase, me],
            device_id={"seq": peer}, device_id_type=MESH,
        )

    def arrived(phase, ref, peer):
        pltpu.make_async_copy(ref, ref, recv_sem.at[phase, peer]).wait()

    def sent(phase, ref, peer):
        pltpu.make_async_copy(ref, ref, send_sem.at[phase, peer]).wait()

    def rows16(ref, i):
        return ref.at[pl.ds(pl.multiple_of(i * 16, 16), 16)]

    vu_v[0:64, :] = jnp.zeros((64, GROUP_HEADS * HEAD_DIM), bf16)
    absorbed_v[...] = jnp.zeros_like(absorbed_v)
    mixed_v[...] = jnp.zeros_like(mixed_v)
    states_v[...] = jnp.zeros_like(states_v)
    l_hid.wait()
    l_gain.wait()
    states_v[0:ROWS, :] = hid_v[...].astype(f32)
    states = states_v[...]
    gained = (states * gain_v[...]).astype(bf16)
    squares = as_row(jnp.sum(states * states, axis=1, keepdims=True))
    row = iota((16, 128), 0)
    l_wq.wait()
    query_part = jnp.dot(gained, wq_v[...], preferred_element_type=f32)
    for k in range(10):
        part = query_part[:, k * 128 : (k + 1) * 128]
        qa_send[k * 16 : (k + 1) * 16, :] = jnp.where(row == 12, squares, part)
    l_wl.wait()
    latent_part = jnp.dot(gained, wl_v[...], preferred_element_type=f32)
    for k in range(5):
        part = latent_part[:, k * 128 : (k + 1) * 128]
        qa_send[(k + 10) * 16 : (k + 11) * 16, :] = jnp.where(row == 12, squares, part)

    pl.semaphore_wait(barrier, SEQ - 1 + heads_size - 1)

    @pl.loop(1, SEQ)
    def _(j):
        peer = lax.rem(me + j, SEQ)

        @pl.when(peer < PIECES)
        def _():
            over_seq(QUERY_SUM, rows16(qa_send, peer), rows16(qa_recv, me), peer).start()

    @pl.when(me < PIECES)
    def _():
        qa_recv[pl.ds(pl.multiple_of(me * 16, 16), 16), :] = qa_send[
            pl.ds(pl.multiple_of(me * 16, 16), 16), :
        ]

        @pl.loop(1, SEQ)
        def _(j):
            peer = lax.rem(me + j, SEQ)
            arrived(QUERY_SUM, rows16(qa_recv, peer), peer)

        total = qa_recv[0:16, :]
        for i in range(1, SEQ):
            total = total + qa_recv[i * 16 : (i + 1) * 16, :]
        mean = as_column(total[12:13, :], row) / D
        done = (lax.rsqrt(mean + epsilon) * total).astype(bf16).astype(f32)
        qa_all[pl.ds(pl.multiple_of(me * 16, 16), 16), :] = jnp.where(row < ROWS, done, 0.0)

        @pl.loop(1, SEQ)
        def _(j):
            peer = lax.rem(me + j, SEQ)
            over_seq(QUERY_ALL, rows16(qa_all, me), rows16(qa_all, me), peer).start()

    @pl.loop(1, SEQ)
    def _(j):
        peer = lax.rem(me + j, SEQ)

        @pl.when(peer < PIECES)
        def _():
            arrived(QUERY_ALL, rows16(qa_all, peer), peer)

    l_ku.wait()
    for k in range(GROUP_HEADS):
        query = qa_all[k * 16 : (k + 1) * 16, :].astype(bf16)
        absorbed = lax.dot_general(
            query, ku_v[:, k * 128 : (k + 1) * 128], (((1,), (1,)), ((), ())),
            preferred_element_type=f32,
        )
        absorbed = absorbed.astype(bf16).astype(f32)
        absorbed_v[0, k * 16 : (k + 1) * 16, :] = absorbed[:, 0:128]
        absorbed_v[1, k * 16 : (k + 1) * 16, :] = absorbed[:, 128:256]
        absorbed_v[2, k * 16 : (k + 1) * 16, 0:64] = absorbed[:, 256:320]

    l_len.wait()
    l_cache.wait()
    positions = me * SPAN + iota((16, SPAN), 1)
    lane = iota((16, 128), 1)
    maxima = jnp.zeros((16, 128), f32)
    totals = jnp.zeros((16, 128), f32)
    scores = []
    for b in range(ROWS):
        one = jnp.concatenate(
            [absorbed_v[t, pl.ds(b, 16, stride=16), :] for t in range(3)], axis=1
        ).astype(bf16)
        scores.append(
            lax.dot_general(
                one, cache_v[b, :, 0:384], (((1,), (1,)), ((), ())), preferred_element_type=f32
            )
        )
    weights = []
    for b in range(ROWS):
        live = positions < len_s[b]
        score = jnp.where(live, scores[b] * scaling, negative_fill)
        top = jnp.max(score, axis=1, keepdims=True)
        weight = jnp.where(live, jnp.exp(score - top), 0.0)
        maxima = jnp.where(lane == b, top, maxima)
        totals = jnp.where(lane == b, jnp.sum(weight, axis=1, keepdims=True), totals)
        weights.append(weight.astype(bf16))
    for b in range(ROWS):
        mixed = jnp.dot(weights[b], cache_v[b, :, 256:640], preferred_element_type=f32)
        for t in range(3):
            mixed_v[t, b * 16 : (b + 1) * 16, :] = mixed[:, t * 128 : (t + 1) * 128]

    l_vu.wait()
    for k in range(GROUP_HEADS):
        mixed = jnp.concatenate(
            [mixed_v[t, pl.ds(k, 16, stride=16), :] for t in range(3)], axis=1
        )
        high = mixed.astype(bf16)
        low = (mixed - high.astype(f32)).astype(bf16)
        both = jnp.dot(
            jnp.concatenate([high, low], axis=0), vu_v[:, k * 128 : (k + 1) * 128],
            preferred_element_type=f32,
        )
        part = both[0:16] + both[16:32]
        part = jnp.where(row == 12, maxima[k : k + 1, :], part)
        part = jnp.where(row == 13, totals[k : k + 1, :], part)
        hb_send[k * 16 : (k + 1) * 16, :] = part

    @pl.loop(1, SEQ)
    def _(j):
        peer = lax.rem(me + j, SEQ)

        @pl.when(owns_head(peer))
        def _():
            over_seq(
                HEAD_SUM, rows16(hb_send, head_of_owner(peer)), rows16(hb_recv, me), peer
            ).start()

    own_key = jnp.concatenate([qa_all[(10 + t) * 16 : (11 + t) * 16, :] for t in range(3)], axis=1)
    own_value = jnp.concatenate(
        [qa_all[(12 + t) * 16 : (13 + t) * 16, :] for t in range(3)], axis=1
    ).astype(bf16)
    own = jnp.dot(own_value, vu_v[...], preferred_element_type=f32)
    for k in range(GROUP_HEADS):
        own_v[k * 16 : (k + 1) * 16, :] = own[:, k * 128 : (k + 1) * 128]

    @pl.when(owns_head(me))
    def _():
        k = head_of_owner(me)
        mine = pl.ds(pl.multiple_of(k * 16, 16), 16)
        hb_recv[pl.ds(pl.multiple_of(me * 16, 16), 16), :] = hb_send[mine, :]
        absorbed = jnp.concatenate([absorbed_v[t, mine, :] for t in range(3)], axis=1)
        own_score = jnp.sum(absorbed * own_key, axis=1, keepdims=True) * scaling

        @pl.loop(1, SEQ)
        def _(j):
            peer = lax.rem(me + j, SEQ)
            arrived(HEAD_SUM, rows16(hb_recv, peer), peer)

        tops = hb_recv[pl.ds(12, 16, stride=16), :].T[0:16, :]
        sums = hb_recv[pl.ds(13, 16, stride=16), :].T[0:16, :]
        highest = jnp.maximum(jnp.max(tops, axis=1, keepdims=True), own_score)
        shares = jnp.exp(tops - highest)
        own_weight = jnp.exp(own_score - highest)
        denominator = jnp.sum(shares * sums, axis=1, keepdims=True) + own_weight
        total = own_weight * own_v[mine, :]
        for i in range(SEQ):
            total = total + shares[:, i : i + 1] * hb_recv[i * 16 : (i + 1) * 16, :]
        head_out = (total / denominator).astype(bf16).astype(f32)
        hb_all[mine, :] = jnp.where(row < ROWS, head_out, 0.0)

        @pl.loop(1, SEQ)
        def _(j):
            peer = lax.rem(me + j, SEQ)
            over_seq(HEAD_ALL, rows16(hb_all, k), rows16(hb_all, k), peer).start()

    @pl.loop(1, SEQ)
    def _(j):
        peer = lax.rem(me + j, SEQ)

        @pl.when(owns_head(peer))
        def _():
            arrived(HEAD_ALL, rows16(hb_all, head_of_owner(peer)), peer)

    def over_heads(phase, src, dst, peer):
        return pltpu.make_async_remote_copy(
            src_ref=src, dst_ref=dst,
            send_sem=x_send_sem.at[phase, peer], recv_sem=x_recv_sem.at[phase, hme],
            device_id={"heads": peer}, device_id_type=MESH,
        )

    l_wo.wait()
    heads_out = jnp.concatenate(
        [hb_all[k * 16 : (k + 1) * 16, :] for k in range(GROUP_HEADS)], axis=1
    ).astype(bf16)
    at_send[...] = jnp.dot(heads_out, wo_v[...], preferred_element_type=f32)
    for j in range(1, heads_size):
        peer = lax.rem(hme + j, heads_size)
        over_heads(0, at_send, at_recv.at[hme], peer).start()
    at_recv[hme] = at_send[...]
    l_fgain.wait()
    for j in range(1, heads_size):
        peer = lax.rem(hme + j, heads_size)
        pltpu.make_async_copy(at_send, at_send, x_recv_sem.at[0, peer]).wait()
    attn = at_recv[0]
    for h in range(1, heads_size):
        attn = attn + at_recv[h]
    updated = states_v[...] + attn
    new_hidden[...] = updated[0:ROWS].astype(bf16)
    sq_send[...] = as_row(jnp.sum(updated * updated, axis=1, keepdims=True))

    @pl.loop(1, SEQ)
    def _(j):
        peer = lax.rem(me + j, SEQ)
        over_seq(SQUARES, sq_send, sq_recv.at[me], peer).start()

    scaled = updated * fgain_v[...]
    bottom = scaled[8:16]
    bottom = jnp.where(iota(bottom.shape, 0) < 4, bottom, pltpu.roll(bottom, 4, 0))
    twice = jnp.concatenate([scaled[0:8], bottom], axis=0).astype(bf16)
    l_wv.wait()
    lower = iota((8, 256), 0) < 4

    def piece(c):
        terms = jnp.dot(
            twice, wv_v[:, pl.ds(pl.multiple_of(c * WIDE, WIDE), WIDE)], preferred_element_type=f32
        )
        vd_send[c, :, 0:512] = terms[0:8]
        vd_send[c, :, 512:768] = jnp.where(lower, terms[8:16, 0:256], terms[8:16, 256:512])

    def last_piece():
        terms = jnp.dot(twice, wv_v[:, 15 * WIDE : VOCAB_LOCAL], preferred_element_type=f32)
        vd_send[15] = jnp.zeros((8, 768), f32)
        vd_send[15, :, 0:TAIL] = terms[0:8]
        vd_send[15, 0:4, 512:768] = terms[8:12, 0:256]
        vd_send[15, 4:8, 512 : 512 + TAIL - 256] = terms[12:16, 256:TAIL]

    def any_piece(c):
        @pl.when(c < 15)
        def _():
            piece(c)

        @pl.when(c == 15)
        def _():
            last_piece()

    @pl.loop(1, SEQ)
    def _(j):
        peer = lax.rem(me + j, SEQ)
        any_piece(peer)
        over_seq(VOCAB_SUM, vd_send.at[peer], vd_recv.at[me], peer).start()

    any_piece(me)
    vd_recv[me] = vd_send[me]
    sq_recv[me] = sq_send[...]

    @pl.loop(1, SEQ)
    def _(j):
        peer = lax.rem(me + j, SEQ)
        arrived(SQUARES, sq_recv.at[peer], peer)
        arrived(VOCAB_SUM, vd_recv.at[peer], peer)

    square_total = sq_recv[0]
    share = vd_recv[0]
    for i in range(1, SEQ):
        square_total = square_total + sq_recv[i]
        share = share + vd_recv[i]
    inv = lax.rsqrt(square_total / D + epsilon)
    sub = iota((8, 128), 0)
    inv_top = as_column(inv, sub)
    inv_bottom = as_column(inv, 8 + lax.rem(sub, 4))
    spot = iota((8, 512), 1)
    spot_bottom = iota((8, 256), 1) + jnp.where(lower, 0, 256)
    limit = VOCAB_LOCAL - me * WIDE
    vd_all[me, :, 0:512] = jnp.where(spot < limit, share[:, 0:512] * inv_top, negative_fill)
    vd_all[me, :, 512:768] = jnp.where(
        spot_bottom < limit, share[:, 512:768] * inv_bottom, negative_fill
    )

    @pl.loop(1, SEQ)
    def _(j):
        peer = lax.rem(me + j, SEQ)
        over_seq(VOCAB_ALL, vd_all.at[me], vd_all.at[me], peer).start()

    l_draft.wait()
    sub1 = iota((8, 1), 0)
    draft_top = jnp.zeros((8, 1), jnp.int32)
    draft_bottom = jnp.zeros((8, 1), jnp.int32)
    for b in range(8):
        draft_top = jnp.where(sub1 == b, draft_s[b], draft_top)
    for b in range(4):
        draft_bottom = jnp.where(lax.rem(sub1, 4) == b, draft_s[8 + b], draft_bottom)
    draft_top = draft_top - hme * VOCAB_LOCAL
    draft_bottom = draft_bottom - hme * VOCAB_LOCAL

    @pl.loop(1, SEQ)
    def _(j):
        peer = lax.rem(me + j, SEQ)
        arrived(VOCAB_ALL, vd_all.at[peer], peer)

    top = vd_all[0]
    for c in range(1, SEQ):
        top = jnp.maximum(top, vd_all[c])
    max_top = jnp.max(top[:, 0:512], axis=1, keepdims=True)
    max_bottom = jnp.max(top[:, 512:768], axis=1, keepdims=True)
    max_bottom = jnp.maximum(max_bottom, pltpu.roll(jnp.broadcast_to(max_bottom, (8, 128)), 4, 0)[:, 0:1])
    sum_top = jnp.zeros((8, 512), f32)
    sum_bottom = jnp.zeros((8, 256), f32)
    pick_top = jnp.zeros((8, 512), f32)
    pick_bottom = jnp.zeros((8, 256), f32)
    for c in range(SEQ):
        high = vd_all[c, :, 0:512]
        low = vd_all[c, :, 512:768]
        sum_top = sum_top + jnp.exp(high - max_top)
        sum_bottom = sum_bottom + jnp.exp(low - max_bottom)
        inside = c * WIDE + spot
        pick_top = pick_top + jnp.where((inside == draft_top) & (inside < VOCAB_LOCAL), high, 0.0)
        inside = c * WIDE + spot_bottom
        pick_bottom = pick_bottom + jnp.where(
            (inside == draft_bottom) & (inside < VOCAB_LOCAL), low, 0.0
        )

    def folded(value):
        column = jnp.sum(value, axis=1, keepdims=True)
        wide = jnp.broadcast_to(column, (8, 128))
        return (wide + pltpu.roll(wide, 4, 0))[:, 0:1]

    lane8 = iota((8, 128), 1)
    block = jnp.zeros((8, 128), f32)
    for i, column in enumerate((
        max_top, max_bottom,
        jnp.sum(sum_top, axis=1, keepdims=True), folded(sum_bottom),
        jnp.sum(pick_top, axis=1, keepdims=True), folded(pick_bottom),
    )):
        block = jnp.where(lane8 == i, column, block)
    st_send[...] = block
    for j in range(1, heads_size):
        peer = lax.rem(hme + j, heads_size)
        over_heads(1, st_send, st_recv.at[hme], peer).start()
    st_recv[hme] = block
    for j in range(1, heads_size):
        peer = lax.rem(hme + j, heads_size)
        pltpu.make_async_copy(st_send, st_send, x_recv_sem.at[1, peer]).wait()
    blocks = [st_recv[h] for h in range(heads_size)]

    def closing(at):
        tops = [x[:, at : at + 1] for x in blocks]
        highest = functools.reduce(jnp.maximum, tops)
        total = sum(x[:, 2 + at : 3 + at] * jnp.exp(t - highest) for x, t in zip(blocks, tops))
        picked = sum(x[:, 4 + at : 5 + at] for x in blocks)
        log_total = highest + jnp.log(total)
        return log_total, picked - log_total

    log_top, picked_top = closing(0)
    log_bottom, picked_bottom = closing(1)
    pick = jnp.where(lane8 == sub, picked_top, 0.0) + jnp.where(
        (lane8 == sub + 8) & (sub < 4), picked_bottom, 0.0
    )
    draft_out[...] = jnp.sum(pick, axis=0, keepdims=True)
    for c in range(SEQ):
        at = c * WIDE
        width = min(WIDE, VOCAB_LOCAL - at)
        log_probs[0:8, at : at + width] = vd_all[c, :, 0:width] - log_top
        low = vd_all[c, :, 512:768] - log_bottom
        log_probs[8:12, at : at + 256] = low[0:4]
        rest = min(256, width - 256)
        log_probs[8:12, at + 256 : at + 256 + rest] = pltpu.roll(low, 4, 0)[0:4, 0:rest]

    @pl.loop(1, SEQ)
    def _(j):
        peer = lax.rem(me + j, SEQ)

        @pl.when(peer < PIECES)
        def _():
            sent(QUERY_SUM, rows16(qa_send, peer), peer)

        @pl.when(me < PIECES)
        def _():
            sent(QUERY_ALL, rows16(qa_all, me), peer)

        @pl.when(owns_head(peer))
        def _():
            sent(HEAD_SUM, rows16(hb_send, head_of_owner(peer)), peer)

        @pl.when(owns_head(me))
        def _():
            sent(HEAD_ALL, rows16(hb_all, head_of_owner(me)), peer)

        sent(SQUARES, sq_send, peer)
        sent(VOCAB_SUM, vd_send.at[peer], peer)
        sent(VOCAB_ALL, vd_all.at[me], peer)

    for j in range(1, heads_size):
        peer = lax.rem(hme + j, heads_size)
        pltpu.make_async_copy(at_send, at_send, x_send_sem.at[0, peer]).wait()
        pltpu.make_async_copy(st_send, st_send, x_send_sem.at[1, peer]).wait()


def solution(mesh):
    heads_size = mesh.shape["heads"]

    def body(hidden, lengths, drafts, gain, wq, wl, cache, ku, vu, wo, fgain, wv):
        any_spec = pl.BlockSpec(memory_space=pl.ANY)
        vmem = pl.BlockSpec(memory_space=pltpu.VMEM)
        width = GROUP_HEADS * HEAD_DIM
        new_hidden, log_probs, draft = pl.pallas_call(
            functools.partial(kernel, heads_size),
            name="decode_step",
            out_shape=(
                jax.ShapeDtypeStruct((ROWS, RANK), bf16),
                jax.ShapeDtypeStruct((ROWS, VOCAB_LOCAL), f32),
                jax.ShapeDtypeStruct((1, 128), f32),
            ),
            in_specs=[any_spec] * 12,
            out_specs=(vmem, vmem, vmem),
            scratch_shapes=[
                pltpu.VMEM((ROWS, RANK), bf16),
                pltpu.SMEM((ROWS,), jnp.int32),
                pltpu.SMEM((ROWS,), jnp.int32),
                pltpu.VMEM((1, RANK), f32),
                pltpu.VMEM((RANK, width), bf16),
                pltpu.VMEM((RANK, 2 * RANK), bf16),
                pltpu.VMEM((ROWS, SPAN, 2 * RANK), bf16),
                pltpu.VMEM((RANK, width), bf16),
                pltpu.VMEM((384, width), bf16),
                pltpu.VMEM((width, RANK), bf16),
                pltpu.VMEM((1, RANK), f32),
                pltpu.VMEM((RANK, VOCAB_LOCAL), bf16),
                pltpu.VMEM((16, RANK), f32),
                pltpu.VMEM((256, 128), f32),
                pltpu.VMEM((256, 128), f32),
                pltpu.VMEM((256, 128), f32),
                pltpu.VMEM((3, 256, 128), f32),
                pltpu.VMEM((3, 256, 128), f32),
                pltpu.VMEM((160, 128), f32),
                pltpu.VMEM((256, 128), f32),
                pltpu.VMEM((160, 128), f32),
                pltpu.VMEM((160, 128), f32),
                pltpu.VMEM((16, RANK), f32),
                pltpu.VMEM((heads_size, 16, RANK), f32),
                pltpu.VMEM((1, 128), f32),
                pltpu.VMEM((SEQ, 1, 128), f32),
                pltpu.VMEM((SEQ, 8, 768), f32),
                pltpu.VMEM((SEQ, 8, 768), f32),
                pltpu.VMEM((SEQ, 8, 768), f32),
                pltpu.VMEM((8, 128), f32),
                pltpu.VMEM((heads_size, 8, 128), f32),
                pltpu.SemaphoreType.DMA((12,)),
                pltpu.SemaphoreType.DMA((7, SEQ)),
                pltpu.SemaphoreType.DMA((7, SEQ)),
                pltpu.SemaphoreType.DMA((2, heads_size)),
                pltpu.SemaphoreType.DMA((2, heads_size)),
            ],
            compiler_params=pltpu.CompilerParams(
                collective_id=0, has_side_effects=True, vmem_limit_bytes=48 * 1024 * 1024
            ),
        )(
            hidden, lengths, drafts, gain.reshape(1, RANK), wq, wl.reshape(RANK, 2 * RANK),
            cache.reshape(ROWS, SPAN, 2 * RANK), ku.reshape(RANK, width), vu.reshape(RANK, width),
            wo, fgain.reshape(1, RANK), wv,
        )
        return new_hidden, log_probs, draft[0, :ROWS]

    return jax.shard_map(
        body,
        mesh=mesh,
        in_specs=(
            P("batch", "seq"), P("batch"), P("batch"), P("seq"), P("seq", "heads"),
            P("seq", "heads", None), P("batch", "heads", "seq", None), P("heads", None, None),
            P("heads", None, None), P("heads", "seq"), P("seq"), P("seq", "heads"),
        ),
        out_specs=(P("batch", "seq"), P("batch", "heads"), P("batch")),
        check_vma=False,
    )
```

```python
import functools
import math

import jax
import jax.numpy as jnp
from jax import lax
from jax.experimental import pallas as pl
from jax.experimental.pallas import tpu as pltpu
from jax.sharding import PartitionSpec as P

D = 5120
HEAD_DIM = 128
GROUP_HEADS = 10
RANK = 320
SEQ = 16
ROWS = 12
SPAN = 256
WIDE = 512
VOCAB_LOCAL = 8000
PIECES = 15
TAIL = VOCAB_LOCAL - 15 * WIDE

MESH = pl.DeviceIdType.MESH
f32 = jnp.float32
bf16 = jnp.bfloat16
epsilon = 1e-05
negative_fill = -1e30
scaling = 1.0 / math.sqrt(HEAD_DIM)

QUERY_SUM, QUERY_ALL, HEAD_SUM, HEAD_ALL, SQUARES, VOCAB_SUM, VOCAB_ALL, STATS = range(8)


def owner_of_head(k):
    return lax.div(k * 8, 5)


def head_of_owner(s):
    return lax.div(s * 5 + 7, 8)


def owns_head(s):
    return owner_of_head(head_of_owner(s)) == s


def iota(shape, dim):
    return lax.broadcasted_iota(jnp.int32, shape, dim)


def as_row(column):
    spread = jnp.where(iota((16, 128), 0) == iota((16, 128), 1), column, 0.0)
    return jnp.sum(spread, axis=0, keepdims=True)


def as_column(row, picks):
    return jnp.sum(jnp.where(picks == iota(picks.shape, 1), row, 0.0), axis=1, keepdims=True)


def kernel(
    heads_size,
    hidden, lengths, drafts, gain, wq, wl, cache, ku, vu, wo, fgain, wv,
    new_hidden, vd_all, logs_out, draft_out,
    hid_v, len_s, draft_s, gain_v, wq_v, wl_v, cache_v, ku_v, vu_v, wo_v, fgain_v, wv_v,
    states_v,
    qa_send, qa_recv, qa_all,
    absorbed_v, mixed_v,
    hb_send, hb_recv, hb_all, own_v,
    at_send, at_recv,
    sq_send, sq_recv,
    vd_send, vd_recv,
    st_send, st_recv,
    load_sem, send_sem, recv_sem, x_send_sem, x_recv_sem,
):
    me = lax.axis_index("seq")
    hme = lax.axis_index("heads")

    def peer_at(j):
        t = lax.div(j, 2)
        over_z = 4 + (1 - 2 * lax.rem(t, 2)) * lax.div(t + 1, 2)
        y, z = lax.div(me, 8), lax.rem(me, 8)
        return lax.rem(y + 1 - lax.rem(j, 2), 2) * 8 + lax.rem(z + over_z, 8)

    def each_peer(step, start=0, stop=SEQ - 1):
        @pl.loop(start, stop)
        def _(j):
            step(peer_at(j))

    barrier = pltpu.get_barrier_semaphore()

    @each_peer
    def _(peer):
        pl.semaphore_signal(barrier, inc=1, device_id={"seq": peer}, device_id_type=MESH)

    for j in range(1, heads_size):
        pl.semaphore_signal(
            barrier, inc=1, device_id={"heads": lax.rem(hme + j, heads_size)}, device_id_type=MESH
        )

    loads = [
        (hidden, hid_v), (gain, gain_v), (lengths, len_s), (drafts, draft_s), (fgain, fgain_v),
        (wq, wq_v), (wl, wl_v), (ku, ku_v), (cache, cache_v), (vu, vu_v.at[pl.ds(64, RANK)]),
        (wo, wo_v), (wv, wv_v),
    ]
    loads = [pltpu.make_async_copy(a, b, load_sem.at[i]) for i, (a, b) in enumerate(loads)]
    l_hid, l_gain, l_len, l_draft, l_fgain, l_wq, l_wl, l_ku, l_cache, l_vu, l_wo, l_wv = loads
    for load in loads:
        load.start()

    def over_seq(phase, src, dst, peer):
        return pltpu.make_async_remote_copy(
            src_ref=src, dst_ref=dst,
            send_sem=send_sem.at[phase], recv_sem=recv_sem.at[phase],
            device_id={"seq": peer}, device_id_type=MESH,
        )

    def arrived(phase, ref, count):
        ref = ref.at[pl.ds(0, count)]
        pltpu.make_async_copy(ref, ref, recv_sem.at[phase]).wait()

    def sent(phase, ref, count):
        ref = ref.at[pl.ds(0, count)]
        pltpu.make_async_copy(ref, ref, send_sem.at[phase]).wait()

    def either(phase, ref, condition, count, waits):
        @pl.when(condition)
        def _():
            waits(phase, ref, count - ref_rows(ref))

        @pl.when(jnp.logical_not(condition))
        def _():
            waits(phase, ref, count)

    def ref_rows(ref):
        return 16 if len(ref.shape) == 2 else 1

    def rows16(ref, i):
        return ref.at[pl.ds(pl.multiple_of(i * 16, 16), 16)]

    vu_v[0:64, :] = jnp.zeros((64, GROUP_HEADS * HEAD_DIM), bf16)
    absorbed_v[...] = jnp.zeros_like(absorbed_v)
    mixed_v[...] = jnp.zeros_like(mixed_v)
    states_v[...] = jnp.zeros_like(states_v)
    l_hid.wait()
    l_gain.wait()
    states_v[0:ROWS, :] = hid_v[...].astype(f32)
    states = states_v[...]
    gained = (states * gain_v[...].reshape(1, RANK)).astype(bf16)
    squares = as_row(jnp.sum(states * states, axis=1, keepdims=True))
    row = iota((16, 128), 0)
    l_wq.wait()
    query_part = jnp.dot(gained, wq_v[...], preferred_element_type=f32)
    for k in range(10):
        part = query_part[:, k * 128 : (k + 1) * 128]
        qa_send[k * 16 : (k + 1) * 16, :] = jnp.where(row == 12, squares, part)
    l_wl.wait()
    latent_part = jnp.dot(gained, wl_v[...], preferred_element_type=f32)
    for k in range(5):
        part = latent_part[:, k * 128 : (k + 1) * 128]
        qa_send[(k + 10) * 16 : (k + 11) * 16, :] = jnp.where(row == 12, squares, part)

    pl.semaphore_wait(barrier, SEQ - 1 + heads_size - 1)

    @each_peer
    def _(peer):
        @pl.when(peer < PIECES)
        def _():
            over_seq(QUERY_SUM, rows16(qa_send, peer), rows16(qa_recv, me), peer).start()

    @pl.when(me < PIECES)
    def _():
        qa_recv[pl.ds(pl.multiple_of(me * 16, 16), 16), :] = qa_send[
            pl.ds(pl.multiple_of(me * 16, 16), 16), :
        ]

        arrived(QUERY_SUM, qa_recv, 15 * 16)

        total = qa_recv[0:16, :]
        for i in range(1, SEQ):
            total = total + qa_recv[i * 16 : (i + 1) * 16, :]
        mean = as_column(total[12:13, :], row) / D
        done = (lax.rsqrt(mean + epsilon) * total).astype(bf16).astype(f32)
        qa_all[pl.ds(pl.multiple_of(me * 16, 16), 16), :] = jnp.where(row < ROWS, done, 0.0)

        @each_peer
        def _(peer):
            over_seq(QUERY_ALL, rows16(qa_all, me), rows16(qa_all, me), peer).start()

    either(QUERY_ALL, qa_all, me < PIECES, PIECES * 16, arrived)

    l_ku.wait()
    for k in range(GROUP_HEADS):
        query = qa_all[k * 16 : (k + 1) * 16, :].astype(bf16)
        absorbed = lax.dot_general(
            query, ku_v[:, k * 128 : (k + 1) * 128], (((1,), (1,)), ((), ())),
            preferred_element_type=f32,
        )
        absorbed = absorbed.astype(bf16).astype(f32)
        absorbed_v[0, k * 16 : (k + 1) * 16, :] = absorbed[:, 0:128]
        absorbed_v[1, k * 16 : (k + 1) * 16, :] = absorbed[:, 128:256]
        absorbed_v[2, k * 16 : (k + 1) * 16, 0:64] = absorbed[:, 256:320]

    l_len.wait()
    l_cache.wait()
    positions = me * SPAN + iota((16, SPAN), 1)
    lane = iota((16, 128), 1)
    maxima = jnp.zeros((16, 128), f32)
    totals = jnp.zeros((16, 128), f32)
    scores = []
    for b in range(ROWS):
        one = jnp.concatenate(
            [absorbed_v[t, pl.ds(b, 16, stride=16), :] for t in range(3)], axis=1
        ).astype(bf16)
        scores.append(
            lax.dot_general(
                one, cache_v[b, :, 0:384], (((1,), (1,)), ((), ())), preferred_element_type=f32
            )
        )
    weights = []
    for b in range(ROWS):
        live = positions < len_s[b]
        score = jnp.where(live, scores[b] * scaling, negative_fill)
        top = jnp.max(score, axis=1, keepdims=True)
        weight = jnp.where(live, jnp.exp(score - top), 0.0)
        maxima = jnp.where(lane == b, top, maxima)
        totals = jnp.where(lane == b, jnp.sum(weight, axis=1, keepdims=True), totals)
        weights.append(weight.astype(bf16))
    for b in range(ROWS):
        mixed = jnp.dot(weights[b], cache_v[b, :, 256:640], preferred_element_type=f32)
        for t in range(3):
            mixed_v[t, b * 16 : (b + 1) * 16, :] = mixed[:, t * 128 : (t + 1) * 128]

    l_vu.wait()
    for k in range(GROUP_HEADS):
        mixed = jnp.concatenate(
            [mixed_v[t, pl.ds(k, 16, stride=16), :] for t in range(3)], axis=1
        )
        high = mixed.astype(bf16)
        low = (mixed - high.astype(f32)).astype(bf16)
        both = jnp.dot(
            jnp.concatenate([high, low], axis=0), vu_v[:, k * 128 : (k + 1) * 128],
            preferred_element_type=f32,
        )
        part = both[0:16] + both[16:32]
        part = jnp.where(row == 12, maxima[k : k + 1, :], part)
        part = jnp.where(row == 13, totals[k : k + 1, :], part)
        hb_send[k * 16 : (k + 1) * 16, :] = part

    @each_peer
    def _(peer):
        @pl.when(owns_head(peer))
        def _():
            over_seq(
                HEAD_SUM, rows16(hb_send, head_of_owner(peer)), rows16(hb_recv, me), peer
            ).start()

    own_key = jnp.concatenate([qa_all[(10 + t) * 16 : (11 + t) * 16, :] for t in range(3)], axis=1)
    own_value = jnp.concatenate(
        [qa_all[(12 + t) * 16 : (13 + t) * 16, :] for t in range(3)], axis=1
    ).astype(bf16)
    own = jnp.dot(own_value, vu_v[...], preferred_element_type=f32)
    for k in range(GROUP_HEADS):
        own_v[k * 16 : (k + 1) * 16, :] = own[:, k * 128 : (k + 1) * 128]

    @pl.when(owns_head(me))
    def _():
        k = head_of_owner(me)
        mine = pl.ds(pl.multiple_of(k * 16, 16), 16)
        hb_recv[pl.ds(pl.multiple_of(me * 16, 16), 16), :] = hb_send[mine, :]
        absorbed = jnp.concatenate([absorbed_v[t, mine, :] for t in range(3)], axis=1)
        own_score = jnp.sum(absorbed * own_key, axis=1, keepdims=True) * scaling

        arrived(HEAD_SUM, hb_recv, 15 * 16)

        tops = hb_recv[pl.ds(12, 16, stride=16), :].T[0:16, :]
        sums = hb_recv[pl.ds(13, 16, stride=16), :].T[0:16, :]
        highest = jnp.maximum(jnp.max(tops, axis=1, keepdims=True), own_score)
        shares = jnp.exp(tops - highest)
        own_weight = jnp.exp(own_score - highest)
        denominator = jnp.sum(shares * sums, axis=1, keepdims=True) + own_weight
        total = own_weight * own_v[mine, :]
        for i in range(SEQ):
            total = total + shares[:, i : i + 1] * hb_recv[i * 16 : (i + 1) * 16, :]
        head_out = (total / denominator).astype(bf16).astype(f32)
        hb_all[mine, :] = jnp.where(row < ROWS, head_out, 0.0)

        @each_peer
        def _(peer):
            over_seq(HEAD_ALL, rows16(hb_all, k), rows16(hb_all, k), peer).start()

    either(HEAD_ALL, hb_all, owns_head(me), GROUP_HEADS * 16, arrived)

    def over_heads(src, dst, peer):
        return pltpu.make_async_remote_copy(
            src_ref=src, dst_ref=dst,
            send_sem=x_send_sem.at[peer], recv_sem=x_recv_sem.at[hme],
            device_id={"heads": peer}, device_id_type=MESH,
        )

    l_wo.wait()
    heads_out = jnp.concatenate(
        [hb_all[k * 16 : (k + 1) * 16, :] for k in range(GROUP_HEADS)], axis=1
    ).astype(bf16)
    at_send[...] = lax.dot_general(
        heads_out, wo_v[...], (((1,), (1,)), ((), ())), preferred_element_type=f32
    )
    for j in range(1, heads_size):
        peer = lax.rem(hme + j, heads_size)
        over_heads(at_send, at_recv.at[hme], peer).start()
    at_recv[hme] = at_send[...]
    l_fgain.wait()
    for j in range(1, heads_size):
        peer = lax.rem(hme + j, heads_size)
        pltpu.make_async_copy(at_send, at_send, x_recv_sem.at[peer]).wait()
    attn = at_recv[0]
    for h in range(1, heads_size):
        attn = attn + at_recv[h]
    updated = states_v[...] + attn
    new_hidden[...] = updated[0:ROWS].astype(bf16)
    sq_send[...] = as_row(jnp.sum(updated * updated, axis=1, keepdims=True))

    @each_peer
    def _(peer):
        over_seq(SQUARES, sq_send, sq_recv.at[me], peer).start()

    scaled = updated * fgain_v[...].reshape(1, RANK)
    bottom = scaled[8:16]
    bottom = jnp.where(iota(bottom.shape, 0) < 4, bottom, pltpu.roll(bottom, 4, 0))
    twice = jnp.concatenate([scaled[0:8], bottom], axis=0).astype(bf16)
    l_wv.wait()
    lower = iota((8, 256), 0) < 4

    def piece(c):
        terms = jnp.dot(
            twice, wv_v[:, pl.ds(pl.multiple_of(c * WIDE, WIDE), WIDE)], preferred_element_type=f32
        )
        vd_send[c, :, 0:512] = terms[0:8]
        vd_send[c, :, 512:768] = jnp.where(lower, terms[8:16, 0:256], terms[8:16, 256:512])

    def last_piece():
        terms = jnp.dot(twice, wv_v[:, 15 * WIDE : VOCAB_LOCAL], preferred_element_type=f32)
        vd_send[15] = jnp.zeros((8, 768), f32)
        vd_send[15, :, 0:TAIL] = terms[0:8]
        vd_send[15, 0:4, 512:768] = terms[8:12, 0:256]
        vd_send[15, 4:8, 512 : 512 + TAIL - 256] = terms[12:16, 256:TAIL]

    def any_piece(c):
        @pl.when(c < 15)
        def _():
            piece(c)

        @pl.when(c == 15)
        def _():
            last_piece()

    @each_peer
    def _(peer):
        any_piece(peer)
        over_seq(VOCAB_SUM, vd_send.at[peer], vd_recv.at[me], peer).start()

    any_piece(me)
    vd_recv[me] = vd_send[me]
    sq_recv[me] = sq_send[...]

    arrived(SQUARES, sq_recv, 15)
    arrived(VOCAB_SUM, vd_recv, 15)

    square_total = sq_recv[0]
    share = vd_recv[0]
    for i in range(1, SEQ):
        square_total = square_total + sq_recv[i]
        share = share + vd_recv[i]
    inv = lax.rsqrt(square_total / D + epsilon)
    sub = iota((8, 128), 0)
    inv_top = as_column(inv, sub)
    inv_bottom = as_column(inv, 8 + lax.rem(sub, 4))
    spot = iota((8, 512), 1)
    spot_bottom = iota((8, 256), 1) + jnp.where(lower, 0, 256)
    limit = VOCAB_LOCAL - me * WIDE
    vd_all[me, :, 0:512] = jnp.where(spot < limit, share[:, 0:512] * inv_top, negative_fill)
    vd_all[me, :, 512:768] = jnp.where(
        spot_bottom < limit, share[:, 512:768] * inv_bottom, negative_fill
    )

    def send_logits(peer):
        over_seq(VOCAB_ALL, vd_all.at[me], vd_all.at[me], peer).start()

    each_peer(send_logits, 0, 4)

    l_draft.wait()
    sub1 = iota((8, 1), 0)
    draft_top = jnp.zeros((8, 1), jnp.int32)
    draft_bottom = jnp.zeros((8, 1), jnp.int32)
    for b in range(8):
        draft_top = jnp.where(sub1 == b, draft_s[b], draft_top)
    for b in range(4):
        draft_bottom = jnp.where(lax.rem(sub1, 4) == b, draft_s[8 + b], draft_bottom)
    first = hme * VOCAB_LOCAL + me * WIDE
    draft_top = draft_top - first
    draft_bottom = draft_bottom - first

    def other_half(column):
        return pltpu.roll(jnp.broadcast_to(column, (8, 128)), 4, 0)[:, 0:1]

    high = vd_all[me, :, 0:512]
    low = vd_all[me, :, 512:768]
    max_top = jnp.max(high, axis=1, keepdims=True)
    max_bottom = jnp.max(low, axis=1, keepdims=True)
    max_bottom = jnp.maximum(max_bottom, other_half(max_bottom))
    sum_top = jnp.sum(jnp.exp(high - max_top), axis=1, keepdims=True)
    sum_bottom = jnp.sum(jnp.exp(low - max_bottom), axis=1, keepdims=True)
    sum_bottom = sum_bottom + other_half(sum_bottom)
    pick_top = jnp.sum(
        jnp.where((spot == draft_top) & (spot < limit), high, 0.0), axis=1, keepdims=True
    )
    pick_bottom = jnp.sum(
        jnp.where((spot_bottom == draft_bottom) & (spot_bottom < limit), low, 0.0),
        axis=1, keepdims=True,
    )
    pick_bottom = pick_bottom + other_half(pick_bottom)

    lane8 = iota((8, 128), 1)
    block = jnp.zeros((8, 128), f32)
    for i, (upper, under) in enumerate(
        ((max_top, max_bottom), (sum_top, sum_bottom), (pick_top, pick_bottom))
    ):
        block = jnp.where(lane8 == sub + 16 * i, upper, block)
        block = jnp.where((lane8 == sub + 16 * i + 8) & (sub < 4), under, block)
    stats = jnp.sum(block, axis=0, keepdims=True)
    st_send[...] = stats
    slot = hme * SEQ + me
    st_recv[slot] = stats

    def send_stats(peer, j):
        pltpu.make_async_remote_copy(
            src_ref=st_send, dst_ref=st_recv.at[slot],
            send_sem=send_sem.at[STATS], recv_sem=recv_sem.at[STATS],
            device_id={"seq": peer, "heads": lax.rem(hme + j, heads_size)}, device_id_type=MESH,
        ).start()

    @each_peer
    def _(peer):
        for j in range(heads_size):
            send_stats(peer, j)

    for j in range(1, heads_size):
        send_stats(me, j)

    each_peer(send_logits, 4, SEQ - 1)

    either(QUERY_SUM, qa_send, me < PIECES, PIECES * 16, sent)

    @pl.when(me < PIECES)
    def _():
        sent(QUERY_ALL, qa_recv, 15 * 16)

    either(HEAD_SUM, hb_send, owns_head(me), GROUP_HEADS * 16, sent)

    @pl.when(owns_head(me))
    def _():
        sent(HEAD_ALL, hb_recv, 15 * 16)

    sent(SQUARES, sq_recv, 15)
    sent(VOCAB_SUM, vd_send, 15)
    for j in range(1, heads_size):
        peer = lax.rem(hme + j, heads_size)
        pltpu.make_async_copy(at_send, at_send, x_send_sem.at[peer]).wait()

    arrived(VOCAB_ALL, vd_all, 15)
    arrived(STATS, st_recv, heads_size * SEQ - 1)
    every = [st_recv[i] for i in range(heads_size * SEQ)]
    highest = functools.reduce(jnp.maximum, every)
    total = jnp.zeros((1, 128), f32)
    picked = jnp.zeros((1, 128), f32)
    for one in every:
        total = total + jnp.exp(one - highest) * pltpu.roll(one, 112, 1)
        picked = picked + one
    log_total = highest + jnp.log(jnp.where(lane8[0:1] < ROWS, total, 1.0))
    draft_out[...] = pltpu.roll(picked, 96, 1) - log_total
    log_top = as_column(log_total, sub)
    log_bottom = as_column(log_total, 8 + lax.rem(sub, 4))
    logs_out[...] = jnp.where(lane8 == 0, log_top, log_bottom)
    sent(VOCAB_ALL, vd_recv, 15)
    sent(STATS, st_recv, heads_size * SEQ - 1)


def closing_kernel(
    new_hidden, logits, logs, draft, hidden_out, probs_out, draft_out, upper_v, lower_v, draft_v, sem
):
    copies = [
        pltpu.make_async_copy(new_hidden, hidden_out, sem.at[0]),
        pltpu.make_async_copy(draft_v, draft_out, sem.at[1]),
        pltpu.make_async_copy(upper_v, probs_out.at[pl.ds(0, 8)], sem.at[2]),
        pltpu.make_async_copy(lower_v, probs_out.at[pl.ds(8, 4)], sem.at[3]),
    ]
    copies[0].start()
    draft_v[...] = draft[...].reshape(128)[:ROWS]
    copies[1].start()
    log_top, log_bottom = logs[:, 0:1], logs[:, 1:2]
    for c in range(SEQ):
        at = c * WIDE
        width = min(WIDE, VOCAB_LOCAL - at)
        upper_v[:, at : at + width] = logits[c, :, 0:width] - log_top
    copies[2].start()
    for c in range(SEQ):
        at = c * WIDE
        low = logits[c, :, 512:768] - log_bottom
        lower_v[:, at : at + 256] = low[0:4]
        rest = min(256, VOCAB_LOCAL - at - 256)
        lower_v[:, at + 256 : at + 256 + rest] = pltpu.roll(low, 4, 0)[0:4, 0:rest]
    copies[3].start()
    for copy in copies:
        copy.wait()


def solution(mesh):
    heads_size = mesh.shape["heads"]

    def body(hidden, lengths, drafts, gain, wq, wl, cache, ku, vu, wo, fgain, wv):
        hbm = pl.BlockSpec(memory_space=pltpu.HBM)
        vmem = pl.BlockSpec(memory_space=pltpu.VMEM)
        width = GROUP_HEADS * HEAD_DIM
        results = pl.pallas_call(
            functools.partial(kernel, heads_size),
            name="decode_step",
            out_shape=(
                jax.ShapeDtypeStruct((ROWS, RANK), bf16),
                jax.ShapeDtypeStruct((SEQ, 8, 768), f32),
                jax.ShapeDtypeStruct((8, 128), f32),
                jax.ShapeDtypeStruct((1, 128), f32),
            ),
            in_specs=[hbm] * 12,
            out_specs=(vmem,) * 4,
            scratch_shapes=[
                pltpu.VMEM((ROWS, RANK), bf16),
                pltpu.SMEM((ROWS,), jnp.int32),
                pltpu.SMEM((ROWS,), jnp.int32),
                pltpu.VMEM((RANK,), f32),
                pltpu.VMEM((RANK, width), bf16),
                pltpu.VMEM((RANK, 2 * RANK), bf16),
                pltpu.VMEM((ROWS, SPAN, 2 * RANK), bf16),
                pltpu.VMEM((RANK, width), bf16),
                pltpu.VMEM((384, width), bf16),
                pltpu.VMEM((RANK, width), bf16),
                pltpu.VMEM((RANK,), f32),
                pltpu.VMEM((RANK, VOCAB_LOCAL), bf16),
                pltpu.VMEM((16, RANK), f32),
                pltpu.VMEM((256, 128), f32),
                pltpu.VMEM((256, 128), f32),
                pltpu.VMEM((256, 128), f32),
                pltpu.VMEM((3, 256, 128), f32),
                pltpu.VMEM((3, 256, 128), f32),
                pltpu.VMEM((160, 128), f32),
                pltpu.VMEM((256, 128), f32),
                pltpu.VMEM((160, 128), f32),
                pltpu.VMEM((160, 128), f32),
                pltpu.VMEM((16, RANK), f32),
                pltpu.VMEM((heads_size, 16, RANK), f32),
                pltpu.VMEM((1, 128), f32),
                pltpu.VMEM((SEQ, 1, 128), f32),
                pltpu.VMEM((SEQ, 8, 768), f32),
                pltpu.VMEM((SEQ, 8, 768), f32),
                pltpu.VMEM((1, 128), f32),
                pltpu.VMEM((heads_size * SEQ, 1, 128), f32),
                pltpu.SemaphoreType.DMA((12,)),
                pltpu.SemaphoreType.DMA((8,)),
                pltpu.SemaphoreType.DMA((8,)),
                pltpu.SemaphoreType.DMA((heads_size,)),
                pltpu.SemaphoreType.DMA((heads_size,)),
            ],
            compiler_params=pltpu.CompilerParams(
                collective_id=0, has_side_effects=True, vmem_limit_bytes=48 * 1024 * 1024
            ),
        )(*(pltpu.with_memory_space_constraint(x, pltpu.HBM) for x in (
            hidden, lengths, drafts, gain, wq, wl.reshape(RANK, 2 * RANK),
            cache.reshape(ROWS, SPAN, 2 * RANK), ku.reshape(RANK, width), vu.reshape(RANK, width),
            wo.T, fgain, wv,
        )))
        return pl.pallas_call(
            closing_kernel,
            name="outputs",
            out_shape=(
                jax.ShapeDtypeStruct((ROWS, RANK), bf16),
                jax.ShapeDtypeStruct((ROWS, VOCAB_LOCAL), f32),
                jax.ShapeDtypeStruct((ROWS,), f32),
            ),
            in_specs=[vmem] * 4,
            out_specs=(hbm,) * 3,
            scratch_shapes=[
                pltpu.VMEM((8, VOCAB_LOCAL), f32),
                pltpu.VMEM((4, VOCAB_LOCAL), f32),
                pltpu.VMEM((ROWS,), f32),
                pltpu.SemaphoreType.DMA((4,)),
            ],
            compiler_params=pltpu.CompilerParams(vmem_limit_bytes=4 * 1024 * 1024),
        )(*results)

    return jax.shard_map(
        body,
        mesh=mesh,
        in_specs=(
            P("batch", "seq"), P("batch"), P("batch"), P("seq"), P("seq", "heads"),
            P("seq", "heads", None), P("batch", "heads", "seq", None), P("heads", None, None),
            P("heads", None, None), P("heads", "seq"), P("seq"), P("seq", "heads"),
        ),
        out_specs=(P("batch", "seq"), P("batch", "heads"), P("batch")),
        check_vma=False,
    )
```

```python
import functools
import math

import jax
import jax.numpy as jnp
from jax import lax
from jax.experimental import pallas as pl
from jax.experimental.pallas import tpu as pltpu
from jax.sharding import PartitionSpec as P

D = 5120
HEAD_DIM = 128
GROUP_HEADS = 10
RANK = 320
SEQ = 16
ROWS = 12
SPAN = 256
WIDE = 512
VOCAB_LOCAL = 8000
PIECES = 15
TAIL = VOCAB_LOCAL - 15 * WIDE

MESH = pl.DeviceIdType.MESH
f32 = jnp.float32
bf16 = jnp.bfloat16
epsilon = 1e-05
negative_fill = -1e30
scaling = 1.0 / math.sqrt(HEAD_DIM)

QUERY_SUM, QUERY_ALL, HEAD_SUM, HEAD_ALL, SQUARES, VOCAB_SUM, VOCAB_ALL, STATS = range(8)


def owner_of_head(k):
    return lax.div(k * 8, 5)


def head_of_owner(s):
    return lax.div(s * 5 + 7, 8)


def owns_head(s):
    return owner_of_head(head_of_owner(s)) == s


def iota(shape, dim):
    return lax.broadcasted_iota(jnp.int32, shape, dim)


def as_row(column):
    spread = jnp.where(iota((16, 128), 0) == iota((16, 128), 1), column, 0.0)
    return jnp.sum(spread, axis=0, keepdims=True)


def as_column(row, picks):
    return jnp.sum(jnp.where(picks == iota(picks.shape, 1), row, 0.0), axis=1, keepdims=True)


def kernel(
    heads_size,
    hidden, lengths, drafts, gain, wq, wl, cache, ku, vu, wo, fgain, wv,
    new_hidden, vd_all, logs_out, draft_out,
    hid_v, len_s, draft_s, gain_v, wq_v, wl_v, cache_v, ku_v, vu_v, wo_v, fgain_v, wv_v,
    states_v,
    qa_send, qa_recv, qa_all,
    absorbed_v, mixed_v,
    hb_send, hb_recv, hb_all, own_v,
    at_send, at_recv,
    sq_send, sq_recv,
    vd_send, vd_recv,
    st_send, st_recv,
    load_sem, send_sem, recv_sem, x_send_sem, x_recv_sem, turn_sem,
):
    me = lax.axis_index("seq")
    hme = lax.axis_index("heads")
    batch = lax.axis_index("batch")
    core = lax.rem(batch, 2)
    partner = batch + 1 - 2 * core

    def peer_at(j):
        t = lax.div(j, 2)
        over_z = 4 + (1 - 2 * lax.rem(t, 2)) * lax.div(t + 1, 2)
        y, z = lax.div(me, 8), lax.rem(me, 8)
        return lax.rem(y + 1 - lax.rem(j, 2), 2) * 8 + lax.rem(z + over_z, 8)

    def each_peer(step, start=0, stop=SEQ - 1):
        @pl.loop(start, stop)
        def _(j):
            step(peer_at(j))

    barrier = pltpu.get_barrier_semaphore()

    @each_peer
    def _(peer):
        pl.semaphore_signal(barrier, inc=1, device_id={"seq": peer}, device_id_type=MESH)

    pl.semaphore_signal(barrier, inc=1, device_id={"batch": partner}, device_id_type=MESH)
    for j in range(1, heads_size):
        pl.semaphore_signal(
            barrier, inc=1, device_id={"heads": lax.rem(hme + j, heads_size)}, device_id_type=MESH
        )

    loads = [
        (hidden, hid_v), (gain, gain_v), (lengths, len_s), (drafts, draft_s), (fgain, fgain_v),
        (wq, wq_v), (wl, wl_v), (ku, ku_v), (cache, cache_v), (vu, vu_v.at[pl.ds(64, RANK)]),
        (wo, wo_v), (wv, wv_v),
    ]
    loads = [pltpu.make_async_copy(a, b, load_sem.at[i]) for i, (a, b) in enumerate(loads)]
    l_hid, l_gain, l_len, l_draft, l_fgain, l_wq, l_wl, l_ku, l_cache, l_vu, l_wo, l_wv = loads
    for load in loads:
        load.start()

    def over_seq(phase, src, dst, peer):
        return pltpu.make_async_remote_copy(
            src_ref=src, dst_ref=dst,
            send_sem=send_sem.at[phase], recv_sem=recv_sem.at[phase],
            device_id={"seq": peer}, device_id_type=MESH,
        )

    def arrived(phase, ref, count):
        ref = ref.at[pl.ds(0, count)]
        pltpu.make_async_copy(ref, ref, recv_sem.at[phase]).wait()

    def sent(phase, ref, count):
        ref = ref.at[pl.ds(0, count)]
        pltpu.make_async_copy(ref, ref, send_sem.at[phase]).wait()

    def either(phase, ref, condition, count, waits):
        @pl.when(condition)
        def _():
            waits(phase, ref, count - ref_rows(ref))

        @pl.when(jnp.logical_not(condition))
        def _():
            waits(phase, ref, count)

    def ref_rows(ref):
        return 16 if len(ref.shape) == 2 else 1

    def rows16(ref, i):
        return ref.at[pl.ds(pl.multiple_of(i * 16, 16), 16)]

    vu_v[0:64, :] = jnp.zeros((64, GROUP_HEADS * HEAD_DIM), bf16)
    absorbed_v[...] = jnp.zeros_like(absorbed_v)
    mixed_v[...] = jnp.zeros_like(mixed_v)
    states_v[...] = jnp.zeros_like(states_v)
    l_hid.wait()
    l_gain.wait()
    states_v[0:ROWS, :] = hid_v[...].astype(f32)
    states = states_v[...]
    gained = (states * gain_v[...].reshape(1, RANK)).astype(bf16)
    squares = as_row(jnp.sum(states * states, axis=1, keepdims=True))
    row = iota((16, 128), 0)
    l_wq.wait()
    query_part = jnp.dot(gained, wq_v[...], preferred_element_type=f32)
    for k in range(10):
        part = query_part[:, k * 128 : (k + 1) * 128]
        qa_send[k * 16 : (k + 1) * 16, :] = jnp.where(row == 12, squares, part)
    l_wl.wait()
    latent_part = jnp.dot(gained, wl_v[...], preferred_element_type=f32)
    for k in range(5):
        part = latent_part[:, k * 128 : (k + 1) * 128]
        qa_send[(k + 10) * 16 : (k + 11) * 16, :] = jnp.where(row == 12, squares, part)

    pl.semaphore_wait(barrier, SEQ + heads_size - 1)

    @each_peer
    def _(peer):
        @pl.when(peer < PIECES)
        def _():
            over_seq(QUERY_SUM, rows16(qa_send, peer), rows16(qa_recv, me), peer).start()

    @pl.when(me < PIECES)
    def _():
        qa_recv[pl.ds(pl.multiple_of(me * 16, 16), 16), :] = qa_send[
            pl.ds(pl.multiple_of(me * 16, 16), 16), :
        ]

        arrived(QUERY_SUM, qa_recv, 15 * 16)

        total = qa_recv[0:16, :]
        for i in range(1, SEQ):
            total = total + qa_recv[i * 16 : (i + 1) * 16, :]
        mean = as_column(total[12:13, :], row) / D
        done = (lax.rsqrt(mean + epsilon) * total).astype(bf16).astype(f32)
        qa_all[pl.ds(pl.multiple_of(me * 16, 16), 16), :] = jnp.where(row < ROWS, done, 0.0)

        @each_peer
        def _(peer):
            over_seq(QUERY_ALL, rows16(qa_all, me), rows16(qa_all, me), peer).start()

    either(QUERY_ALL, qa_all, me < PIECES, PIECES * 16, arrived)

    l_ku.wait()
    for k in range(GROUP_HEADS):
        query = qa_all[k * 16 : (k + 1) * 16, :].astype(bf16)
        absorbed = lax.dot_general(
            query, ku_v[:, k * 128 : (k + 1) * 128], (((1,), (1,)), ((), ())),
            preferred_element_type=f32,
        )
        absorbed = absorbed.astype(bf16).astype(f32)
        absorbed_v[0, k * 16 : (k + 1) * 16, :] = absorbed[:, 0:128]
        absorbed_v[1, k * 16 : (k + 1) * 16, :] = absorbed[:, 128:256]
        absorbed_v[2, k * 16 : (k + 1) * 16, 0:64] = absorbed[:, 256:320]

    l_len.wait()
    l_cache.wait()
    positions = me * SPAN + iota((16, SPAN), 1)
    lane = iota((16, 128), 1)
    maxima = jnp.zeros((16, 128), f32)
    totals = jnp.zeros((16, 128), f32)
    scores = []
    for b in range(ROWS):
        one = jnp.concatenate(
            [absorbed_v[t, pl.ds(b, 16, stride=16), :] for t in range(3)], axis=1
        ).astype(bf16)
        scores.append(
            lax.dot_general(
                one, cache_v[b, :, 0:384], (((1,), (1,)), ((), ())), preferred_element_type=f32
            )
        )
    weights = []
    for b in range(ROWS):
        live = positions < len_s[b]
        score = jnp.where(live, scores[b] * scaling, negative_fill)
        top = jnp.max(score, axis=1, keepdims=True)
        weight = jnp.where(live, jnp.exp(score - top), 0.0)
        maxima = jnp.where(lane == b, top, maxima)
        totals = jnp.where(lane == b, jnp.sum(weight, axis=1, keepdims=True), totals)
        weights.append(weight.astype(bf16))
    for b in range(ROWS):
        mixed = jnp.dot(weights[b], cache_v[b, :, 256:640], preferred_element_type=f32)
        for t in range(3):
            mixed_v[t, b * 16 : (b + 1) * 16, :] = mixed[:, t * 128 : (t + 1) * 128]

    l_vu.wait()
    for k in range(GROUP_HEADS):
        mixed = jnp.concatenate(
            [mixed_v[t, pl.ds(k, 16, stride=16), :] for t in range(3)], axis=1
        )
        high = mixed.astype(bf16)
        low = (mixed - high.astype(f32)).astype(bf16)
        both = jnp.dot(
            jnp.concatenate([high, low], axis=0), vu_v[:, k * 128 : (k + 1) * 128],
            preferred_element_type=f32,
        )
        part = both[0:16] + both[16:32]
        part = jnp.where(row == 12, maxima[k : k + 1, :], part)
        part = jnp.where(row == 13, totals[k : k + 1, :], part)
        hb_send[k * 16 : (k + 1) * 16, :] = part

    @each_peer
    def _(peer):
        @pl.when(owns_head(peer))
        def _():
            over_seq(
                HEAD_SUM, rows16(hb_send, head_of_owner(peer)), rows16(hb_recv, me), peer
            ).start()

    own_key = jnp.concatenate([qa_all[(10 + t) * 16 : (11 + t) * 16, :] for t in range(3)], axis=1)
    own_value = jnp.concatenate(
        [qa_all[(12 + t) * 16 : (13 + t) * 16, :] for t in range(3)], axis=1
    ).astype(bf16)
    own = jnp.dot(own_value, vu_v[...], preferred_element_type=f32)
    for k in range(GROUP_HEADS):
        own_v[k * 16 : (k + 1) * 16, :] = own[:, k * 128 : (k + 1) * 128]

    @pl.when(owns_head(me))
    def _():
        k = head_of_owner(me)
        mine = pl.ds(pl.multiple_of(k * 16, 16), 16)
        hb_recv[pl.ds(pl.multiple_of(me * 16, 16), 16), :] = hb_send[mine, :]
        absorbed = jnp.concatenate([absorbed_v[t, mine, :] for t in range(3)], axis=1)
        own_score = jnp.sum(absorbed * own_key, axis=1, keepdims=True) * scaling

        arrived(HEAD_SUM, hb_recv, 15 * 16)

        tops = hb_recv[pl.ds(12, 16, stride=16), :].T[0:16, :]
        sums = hb_recv[pl.ds(13, 16, stride=16), :].T[0:16, :]
        highest = jnp.maximum(jnp.max(tops, axis=1, keepdims=True), own_score)
        shares = jnp.exp(tops - highest)
        own_weight = jnp.exp(own_score - highest)
        denominator = jnp.sum(shares * sums, axis=1, keepdims=True) + own_weight
        total = own_weight * own_v[mine, :]
        for i in range(SEQ):
            total = total + shares[:, i : i + 1] * hb_recv[i * 16 : (i + 1) * 16, :]
        head_out = (total / denominator).astype(bf16).astype(f32)
        hb_all[mine, :] = jnp.where(row < ROWS, head_out, 0.0)

        @each_peer
        def _(peer):
            over_seq(HEAD_ALL, rows16(hb_all, k), rows16(hb_all, k), peer).start()

    either(HEAD_ALL, hb_all, owns_head(me), GROUP_HEADS * 16, arrived)

    def over_heads(src, dst, peer):
        return pltpu.make_async_remote_copy(
            src_ref=src, dst_ref=dst,
            send_sem=x_send_sem.at[peer], recv_sem=x_recv_sem.at[hme],
            device_id={"heads": peer}, device_id_type=MESH,
        )

    l_wo.wait()
    heads_out = jnp.concatenate(
        [hb_all[k * 16 : (k + 1) * 16, :] for k in range(GROUP_HEADS)], axis=1
    ).astype(bf16)
    at_send[...] = lax.dot_general(
        heads_out, wo_v[...], (((1,), (1,)), ((), ())), preferred_element_type=f32
    )
    for j in range(1, heads_size):
        peer = lax.rem(hme + j, heads_size)
        over_heads(at_send, at_recv.at[hme], peer).start()
    at_recv[hme] = at_send[...]
    l_fgain.wait()
    for j in range(1, heads_size):
        peer = lax.rem(hme + j, heads_size)
        pltpu.make_async_copy(at_send, at_send, x_recv_sem.at[peer]).wait()
    attn = at_recv[0]
    for h in range(1, heads_size):
        attn = attn + at_recv[h]
    updated = states_v[...] + attn
    new_hidden[...] = updated[0:ROWS].astype(bf16)
    sq_send[...] = as_row(jnp.sum(updated * updated, axis=1, keepdims=True))

    @each_peer
    def _(peer):
        over_seq(SQUARES, sq_send, sq_recv.at[me], peer).start()

    scaled = updated * fgain_v[...].reshape(1, RANK)
    bottom = scaled[8:16]
    bottom = jnp.where(iota(bottom.shape, 0) < 4, bottom, pltpu.roll(bottom, 4, 0))
    twice = jnp.concatenate([scaled[0:8], bottom], axis=0).astype(bf16)
    l_wv.wait()
    lower = iota((8, 256), 0) < 4

    def piece(c):
        terms = jnp.dot(
            twice, wv_v[:, pl.ds(pl.multiple_of(c * WIDE, WIDE), WIDE)], preferred_element_type=f32
        )
        vd_send[c, :, 0:512] = terms[0:8]
        vd_send[c, :, 512:768] = jnp.where(lower, terms[8:16, 0:256], terms[8:16, 256:512])

    def last_piece():
        terms = jnp.dot(twice, wv_v[:, 15 * WIDE : VOCAB_LOCAL], preferred_element_type=f32)
        vd_send[15] = jnp.zeros((8, 768), f32)
        vd_send[15, :, 0:TAIL] = terms[0:8]
        vd_send[15, 0:4, 512:768] = terms[8:12, 0:256]
        vd_send[15, 4:8, 512 : 512 + TAIL - 256] = terms[12:16, 256:TAIL]

    def any_piece(c):
        @pl.when(c < 15)
        def _():
            piece(c)

        @pl.when(c == 15)
        def _():
            last_piece()

    @each_peer
    def _(peer):
        any_piece(peer)
        over_seq(VOCAB_SUM, vd_send.at[peer], vd_recv.at[me], peer).start()

    any_piece(me)
    vd_recv[me] = vd_send[me]
    sq_recv[me] = sq_send[...]

    @pl.when(core == 0)
    def _():
        sent(VOCAB_SUM, vd_send, 15)
        pl.semaphore_signal(turn_sem, inc=1, device_id={"batch": partner}, device_id_type=MESH)

    arrived(SQUARES, sq_recv, 15)
    arrived(VOCAB_SUM, vd_recv, 15)

    square_total = sq_recv[0]
    share = vd_recv[0]
    for i in range(1, SEQ):
        square_total = square_total + sq_recv[i]
        share = share + vd_recv[i]
    inv = lax.rsqrt(square_total / D + epsilon)
    sub = iota((8, 128), 0)
    inv_top = as_column(inv, sub)
    inv_bottom = as_column(inv, 8 + lax.rem(sub, 4))
    spot = iota((8, 512), 1)
    spot_bottom = iota((8, 256), 1) + jnp.where(lower, 0, 256)
    limit = VOCAB_LOCAL - me * WIDE
    vd_all[me, :, 0:512] = jnp.where(spot < limit, share[:, 0:512] * inv_top, negative_fill)
    vd_all[me, :, 512:768] = jnp.where(
        spot_bottom < limit, share[:, 512:768] * inv_bottom, negative_fill
    )

    @pl.when(core == 1)
    def _():
        pl.semaphore_wait(turn_sem, 1)

    def send_logits(peer):
        over_seq(VOCAB_ALL, vd_all.at[me], vd_all.at[me], peer).start()

    each_peer(send_logits, 0, 4)

    l_draft.wait()
    sub1 = iota((8, 1), 0)
    draft_top = jnp.zeros((8, 1), jnp.int32)
    draft_bottom = jnp.zeros((8, 1), jnp.int32)
    for b in range(8):
        draft_top = jnp.where(sub1 == b, draft_s[b], draft_top)
    for b in range(4):
        draft_bottom = jnp.where(lax.rem(sub1, 4) == b, draft_s[8 + b], draft_bottom)
    first = hme * VOCAB_LOCAL + me * WIDE
    draft_top = draft_top - first
    draft_bottom = draft_bottom - first

    def other_half(column):
        return pltpu.roll(jnp.broadcast_to(column, (8, 128)), 4, 0)[:, 0:1]

    high = vd_all[me, :, 0:512]
    low = vd_all[me, :, 512:768]
    max_top = jnp.max(high, axis=1, keepdims=True)
    max_bottom = jnp.max(low, axis=1, keepdims=True)
    max_bottom = jnp.maximum(max_bottom, other_half(max_bottom))
    sum_top = jnp.sum(jnp.exp(high - max_top), axis=1, keepdims=True)
    sum_bottom = jnp.sum(jnp.exp(low - max_bottom), axis=1, keepdims=True)
    sum_bottom = sum_bottom + other_half(sum_bottom)
    pick_top = jnp.sum(
        jnp.where((spot == draft_top) & (spot < limit), high, 0.0), axis=1, keepdims=True
    )
    pick_bottom = jnp.sum(
        jnp.where((spot_bottom == draft_bottom) & (spot_bottom < limit), low, 0.0),
        axis=1, keepdims=True,
    )
    pick_bottom = pick_bottom + other_half(pick_bottom)

    lane8 = iota((8, 128), 1)
    block = jnp.zeros((8, 128), f32)
    for i, (upper, under) in enumerate(
        ((max_top, max_bottom), (sum_top, sum_bottom), (pick_top, pick_bottom))
    ):
        block = jnp.where(lane8 == sub + 16 * i, upper, block)
        block = jnp.where((lane8 == sub + 16 * i + 8) & (sub < 4), under, block)
    stats = jnp.sum(block, axis=0, keepdims=True)
    st_send[...] = stats
    slot = hme * SEQ + me
    st_recv[slot] = stats

    def send_stats(peer, j):
        pltpu.make_async_remote_copy(
            src_ref=st_send, dst_ref=st_recv.at[slot],
            send_sem=send_sem.at[STATS], recv_sem=recv_sem.at[STATS],
            device_id={"seq": peer, "heads": lax.rem(hme + j, heads_size)}, device_id_type=MESH,
        ).start()

    @each_peer
    def _(peer):
        for j in range(heads_size):
            send_stats(peer, j)

    for j in range(1, heads_size):
        send_stats(me, j)

    each_peer(send_logits, 4, SEQ - 1)

    either(QUERY_SUM, qa_send, me < PIECES, PIECES * 16, sent)

    @pl.when(me < PIECES)
    def _():
        sent(QUERY_ALL, qa_recv, 15 * 16)

    either(HEAD_SUM, hb_send, owns_head(me), GROUP_HEADS * 16, sent)

    @pl.when(owns_head(me))
    def _():
        sent(HEAD_ALL, hb_recv, 15 * 16)

    sent(SQUARES, sq_recv, 15)

    @pl.when(core == 1)
    def _():
        sent(VOCAB_SUM, vd_send, 15)

    for j in range(1, heads_size):
        peer = lax.rem(hme + j, heads_size)
        pltpu.make_async_copy(at_send, at_send, x_send_sem.at[peer]).wait()

    arrived(VOCAB_ALL, vd_all, 15)
    arrived(STATS, st_recv, heads_size * SEQ - 1)
    every = [st_recv[i] for i in range(heads_size * SEQ)]
    highest = functools.reduce(jnp.maximum, every)
    total = jnp.zeros((1, 128), f32)
    picked = jnp.zeros((1, 128), f32)
    for one in every:
        total = total + jnp.exp(one - highest) * pltpu.roll(one, 112, 1)
        picked = picked + one
    log_total = highest + jnp.log(jnp.where(lane8[0:1] < ROWS, total, 1.0))
    draft_out[...] = pltpu.roll(picked, 96, 1) - log_total
    log_top = as_column(log_total, sub)
    log_bottom = as_column(log_total, 8 + lax.rem(sub, 4))
    logs_out[...] = jnp.where(lane8 == 0, log_top, log_bottom)
    sent(VOCAB_ALL, vd_recv, 15)
    sent(STATS, st_recv, heads_size * SEQ - 1)


def closing_kernel(
    new_hidden, logits, logs, draft, hidden_out, probs_out, draft_out, upper_v, lower_v, draft_v, sem
):
    copies = [
        pltpu.make_async_copy(new_hidden, hidden_out, sem.at[0]),
        pltpu.make_async_copy(draft_v, draft_out, sem.at[1]),
        pltpu.make_async_copy(upper_v, probs_out.at[pl.ds(0, 8)], sem.at[2]),
        pltpu.make_async_copy(lower_v, probs_out.at[pl.ds(8, 4)], sem.at[3]),
    ]
    copies[0].start()
    draft_v[...] = draft[...].reshape(128)[:ROWS]
    copies[1].start()
    log_top, log_bottom = logs[:, 0:1], logs[:, 1:2]
    for c in range(SEQ):
        at = c * WIDE
        width = min(WIDE, VOCAB_LOCAL - at)
        upper_v[:, at : at + width] = logits[c, :, 0:width] - log_top
    copies[2].start()
    for c in range(SEQ):
        at = c * WIDE
        low = logits[c, :, 512:768] - log_bottom
        lower_v[:, at : at + 256] = low[0:4]
        rest = min(256, VOCAB_LOCAL - at - 256)
        lower_v[:, at + 256 : at + 256 + rest] = pltpu.roll(low, 4, 0)[0:4, 0:rest]
    copies[3].start()
    for copy in copies:
        copy.wait()


def solution(mesh):
    heads_size = mesh.shape["heads"]

    def body(hidden, lengths, drafts, gain, wq, wl, cache, ku, vu, wo, fgain, wv):
        hbm = pl.BlockSpec(memory_space=pltpu.HBM)
        vmem = pl.BlockSpec(memory_space=pltpu.VMEM)
        width = GROUP_HEADS * HEAD_DIM
        results = pl.pallas_call(
            functools.partial(kernel, heads_size),
            name="decode_step",
            out_shape=(
                jax.ShapeDtypeStruct((ROWS, RANK), bf16),
                jax.ShapeDtypeStruct((SEQ, 8, 768), f32),
                jax.ShapeDtypeStruct((8, 128), f32),
                jax.ShapeDtypeStruct((1, 128), f32),
            ),
            in_specs=[hbm] * 12,
            out_specs=(vmem,) * 4,
            scratch_shapes=[
                pltpu.VMEM((ROWS, RANK), bf16),
                pltpu.SMEM((ROWS,), jnp.int32),
                pltpu.SMEM((ROWS,), jnp.int32),
                pltpu.VMEM((RANK,), f32),
                pltpu.VMEM((RANK, width), bf16),
                pltpu.VMEM((RANK, 2 * RANK), bf16),
                pltpu.VMEM((ROWS, SPAN, 2 * RANK), bf16),
                pltpu.VMEM((RANK, width), bf16),
                pltpu.VMEM((384, width), bf16),
                pltpu.VMEM((RANK, width), bf16),
                pltpu.VMEM((RANK,), f32),
                pltpu.VMEM((RANK, VOCAB_LOCAL), bf16),
                pltpu.VMEM((16, RANK), f32),
                pltpu.VMEM((256, 128), f32),
                pltpu.VMEM((256, 128), f32),
                pltpu.VMEM((256, 128), f32),
                pltpu.VMEM((3, 256, 128), f32),
                pltpu.VMEM((3, 256, 128), f32),
                pltpu.VMEM((160, 128), f32),
                pltpu.VMEM((256, 128), f32),
                pltpu.VMEM((160, 128), f32),
                pltpu.VMEM((160, 128), f32),
                pltpu.VMEM((16, RANK), f32),
                pltpu.VMEM((heads_size, 16, RANK), f32),
                pltpu.VMEM((1, 128), f32),
                pltpu.VMEM((SEQ, 1, 128), f32),
                pltpu.VMEM((SEQ, 8, 768), f32),
                pltpu.VMEM((SEQ, 8, 768), f32),
                pltpu.VMEM((1, 128), f32),
                pltpu.VMEM((heads_size * SEQ, 1, 128), f32),
                pltpu.SemaphoreType.DMA((12,)),
                pltpu.SemaphoreType.DMA((8,)),
                pltpu.SemaphoreType.DMA((8,)),
                pltpu.SemaphoreType.DMA((heads_size,)),
                pltpu.SemaphoreType.DMA((heads_size,)),
                pltpu.SemaphoreType.REGULAR,
            ],
            compiler_params=pltpu.CompilerParams(
                collective_id=0, has_side_effects=True, vmem_limit_bytes=48 * 1024 * 1024
            ),
        )(*(pltpu.with_memory_space_constraint(x, pltpu.HBM) for x in (
            hidden, lengths, drafts, gain, wq, wl.reshape(RANK, 2 * RANK),
            cache.reshape(ROWS, SPAN, 2 * RANK), ku.reshape(RANK, width), vu.reshape(RANK, width),
            wo.T, fgain, wv,
        )))
        return pl.pallas_call(
            closing_kernel,
            name="outputs",
            out_shape=(
                jax.ShapeDtypeStruct((ROWS, RANK), bf16),
                jax.ShapeDtypeStruct((ROWS, VOCAB_LOCAL), f32),
                jax.ShapeDtypeStruct((ROWS,), f32),
            ),
            in_specs=[vmem] * 4,
            out_specs=(hbm,) * 3,
            scratch_shapes=[
                pltpu.VMEM((8, VOCAB_LOCAL), f32),
                pltpu.VMEM((4, VOCAB_LOCAL), f32),
                pltpu.VMEM((ROWS,), f32),
                pltpu.SemaphoreType.DMA((4,)),
            ],
            compiler_params=pltpu.CompilerParams(vmem_limit_bytes=4 * 1024 * 1024),
        )(*results)

    return jax.shard_map(
        body,
        mesh=mesh,
        in_specs=(
            P("batch", "seq"), P("batch"), P("batch"), P("seq"), P("seq", "heads"),
            P("seq", "heads", None), P("batch", "heads", "seq", None), P("heads", None, None),
            P("heads", None, None), P("heads", "seq"), P("seq"), P("seq", "heads"),
        ),
        out_specs=(P("batch", "seq"), P("batch", "heads"), P("batch")),
        check_vma=False,
    )
```

```python
import functools
import math

import jax
import jax.numpy as jnp
from jax import lax
from jax.experimental import pallas as pl
from jax.experimental.pallas import tpu as pltpu
from jax.sharding import PartitionSpec as P

D = 5120
HEAD_DIM = 128
GROUP_HEADS = 10
RANK = 320
SEQ = 16
ROWS = 12
SPAN = 256
WIDE = 512
VOCAB_LOCAL = 8000
PIECES = 15
NEAR = 3
TAIL = VOCAB_LOCAL - 15 * WIDE

MESH = pl.DeviceIdType.MESH
f32 = jnp.float32
bf16 = jnp.bfloat16
epsilon = 1e-05
negative_fill = -1e30
scaling = 1.0 / math.sqrt(HEAD_DIM)

QUERY_SUM, QUERY_ALL, HEAD_SUM, HEAD_ALL, SQUARES, VOCAB_SUM, VOCAB_ALL, STATS, VOCAB_HALF = range(9)


def owner_of_head(k):
    return lax.div(k * 8, 5)


def head_of_owner(s):
    return lax.div(s * 5 + 7, 8)


def owns_head(s):
    return owner_of_head(head_of_owner(s)) == s


def iota(shape, dim):
    return lax.broadcasted_iota(jnp.int32, shape, dim)


def as_row(column):
    spread = jnp.where(iota((16, 128), 0) == iota((16, 128), 1), column, 0.0)
    return jnp.sum(spread, axis=0, keepdims=True)


def as_column(row, picks):
    return jnp.sum(jnp.where(picks == iota(picks.shape, 1), row, 0.0), axis=1, keepdims=True)


def kernel(
    heads_size,
    hidden, lengths, drafts, gain, wq, wl, cache, ku, vu, wo, fgain, wv,
    new_hidden, vd_all, logs_out, draft_out,
    hid_v, len_s, draft_s, gain_v, wq_v, wl_v, cache_v, ku_v, vu_v, wo_v, fgain_v, wv_v,
    states_v,
    qa_send, qa_recv, qa_all,
    absorbed_v, mixed_v,
    hb_send, hb_recv, hb_all, own_v,
    at_send, at_recv,
    sq_send, sq_recv,
    vd_send, vd_recv, vd_half,
    st_send, st_recv,
    load_sem, send_sem, recv_sem, x_send_sem, x_recv_sem, turn_sem, near_sem, half_sem,
):
    me = lax.axis_index("seq")
    hme = lax.axis_index("heads")
    batch = lax.axis_index("batch")
    core = lax.rem(batch, 2)
    partner = batch + 1 - 2 * core

    def peer_at(j):
        t = lax.div(j, 2)
        over_z = 4 + (1 - 2 * lax.rem(t, 2)) * lax.div(t + 1, 2)
        y, z = lax.div(me, 8), lax.rem(me, 8)
        return lax.rem(y + 1 - lax.rem(j, 2), 2) * 8 + lax.rem(z + over_z, 8)

    def each_peer(step, start=0, stop=SEQ - 1):
        @pl.loop(start, stop)
        def _(j):
            step(peer_at(j))

    barrier = pltpu.get_barrier_semaphore()

    @each_peer
    def _(peer):
        pl.semaphore_signal(barrier, inc=1, device_id={"seq": peer}, device_id_type=MESH)

    pl.semaphore_signal(barrier, inc=1, device_id={"batch": partner}, device_id_type=MESH)
    for j in range(1, heads_size):
        pl.semaphore_signal(
            barrier, inc=1, device_id={"heads": lax.rem(hme + j, heads_size)}, device_id_type=MESH
        )

    loads = [
        (hidden, hid_v), (gain, gain_v), (lengths, len_s), (drafts, draft_s), (fgain, fgain_v),
        (wq, wq_v), (wl, wl_v), (ku, ku_v), (cache, cache_v), (vu, vu_v.at[pl.ds(64, RANK)]),
        (wo, wo_v), (wv, wv_v),
    ]
    loads = [pltpu.make_async_copy(a, b, load_sem.at[i]) for i, (a, b) in enumerate(loads)]
    l_hid, l_gain, l_len, l_draft, l_fgain, l_wq, l_wl, l_ku, l_cache, l_vu, l_wo, l_wv = loads
    for load in loads:
        load.start()

    def over_seq(phase, src, dst, peer):
        return pltpu.make_async_remote_copy(
            src_ref=src, dst_ref=dst,
            send_sem=send_sem.at[phase], recv_sem=recv_sem.at[phase],
            device_id={"seq": peer}, device_id_type=MESH,
        )

    def arrived(phase, ref, count):
        ref = ref.at[pl.ds(0, count)]
        pltpu.make_async_copy(ref, ref, recv_sem.at[phase]).wait()

    def sent(phase, ref, count):
        ref = ref.at[pl.ds(0, count)]
        pltpu.make_async_copy(ref, ref, send_sem.at[phase]).wait()

    def rows(ref, i, count):
        return ref.at[pl.ds(pl.multiple_of(i * 16, 16), count)]

    def either(phase, ref, condition, count, size, waits):
        @pl.when(condition)
        def _():
            waits(phase, ref, (count - 1) * size)

        @pl.when(jnp.logical_not(condition))
        def _():
            waits(phase, ref, count * size)

    vu_v[0:64, :] = jnp.zeros((64, GROUP_HEADS * HEAD_DIM), bf16)
    absorbed_v[...] = jnp.zeros_like(absorbed_v)
    mixed_v[...] = jnp.zeros_like(mixed_v)
    states_v[...] = jnp.zeros_like(states_v)
    l_hid.wait()
    l_gain.wait()
    states_v[0:ROWS, :] = hid_v[...].astype(f32)
    states = states_v[...]
    gained = (states * gain_v[...].reshape(1, RANK)).astype(bf16)
    squares = as_row(jnp.sum(states * states, axis=1, keepdims=True))
    row = iota((16, 128), 0)
    l_wq.wait()
    query_part = jnp.dot(gained, wq_v[...], preferred_element_type=f32)
    for k in range(10):
        part = query_part[:, k * 128 : (k + 1) * 128]
        qa_send[k * 16 : (k + 1) * 16, :] = jnp.where(row == 12, squares, part)
    l_wl.wait()
    latent_part = jnp.dot(gained, wl_v[...], preferred_element_type=f32)
    for k in range(5):
        part = latent_part[:, k * 128 : (k + 1) * 128]
        qa_send[(k + 10) * 16 : (k + 11) * 16, :] = jnp.where(row == 12, squares, part)

    pl.semaphore_wait(barrier, SEQ + heads_size - 1)

    @each_peer
    def _(peer):
        @pl.when(peer < PIECES)
        def _():
            over_seq(QUERY_SUM, rows(qa_send, peer, 13), rows(qa_recv, me, 13), peer).start()

    @pl.when(me < PIECES)
    def _():
        qa_recv[pl.ds(pl.multiple_of(me * 16, 16), 16), :] = qa_send[
            pl.ds(pl.multiple_of(me * 16, 16), 16), :
        ]

        arrived(QUERY_SUM, qa_recv, 15 * 13)

        total = qa_recv[0:16, :]
        for i in range(1, SEQ):
            total = total + qa_recv[i * 16 : (i + 1) * 16, :]
        mean = as_column(total[12:13, :], row) / D
        done = (lax.rsqrt(mean + epsilon) * total).astype(bf16).astype(f32)
        qa_all[pl.ds(pl.multiple_of(me * 16, 16), 16), :] = jnp.where(row < ROWS, done, 0.0)

        @each_peer
        def _(peer):
            over_seq(QUERY_ALL, rows(qa_all, me, ROWS), rows(qa_all, me, ROWS), peer).start()

    either(QUERY_ALL, qa_all, me < PIECES, PIECES, ROWS, arrived)

    l_ku.wait()
    for k in range(GROUP_HEADS):
        query = qa_all[k * 16 : (k + 1) * 16, :].astype(bf16)
        absorbed = lax.dot_general(
            query, ku_v[:, k * 128 : (k + 1) * 128], (((1,), (1,)), ((), ())),
            preferred_element_type=f32,
        )
        absorbed = absorbed.astype(bf16).astype(f32)
        absorbed_v[0, k * 16 : (k + 1) * 16, :] = absorbed[:, 0:128]
        absorbed_v[1, k * 16 : (k + 1) * 16, :] = absorbed[:, 128:256]
        absorbed_v[2, k * 16 : (k + 1) * 16, 0:64] = absorbed[:, 256:320]

    l_len.wait()
    l_cache.wait()
    positions = me * SPAN + iota((16, SPAN), 1)
    lane = iota((16, 128), 1)
    maxima = jnp.zeros((16, 128), f32)
    totals = jnp.zeros((16, 128), f32)
    scores = []
    for b in range(ROWS):
        one = jnp.concatenate(
            [absorbed_v[t, pl.ds(b, 16, stride=16), :] for t in range(3)], axis=1
        ).astype(bf16)
        scores.append(
            lax.dot_general(
                one, cache_v[b, :, 0:384], (((1,), (1,)), ((), ())), preferred_element_type=f32
            )
        )
    weights = []
    for b in range(ROWS):
        live = positions < len_s[b]
        score = jnp.where(live, scores[b] * scaling, negative_fill)
        top = jnp.max(score, axis=1, keepdims=True)
        weight = jnp.where(live, jnp.exp(score - top), 0.0)
        maxima = jnp.where(lane == b, top, maxima)
        totals = jnp.where(lane == b, jnp.sum(weight, axis=1, keepdims=True), totals)
        weights.append(weight.astype(bf16))
    for b in range(ROWS):
        mixed = jnp.dot(weights[b], cache_v[b, :, 256:640], preferred_element_type=f32)
        for t in range(3):
            mixed_v[t, b * 16 : (b + 1) * 16, :] = mixed[:, t * 128 : (t + 1) * 128]

    l_vu.wait()
    for k in range(GROUP_HEADS):
        mixed = jnp.concatenate(
            [mixed_v[t, pl.ds(k, 16, stride=16), :] for t in range(3)], axis=1
        )
        high = mixed.astype(bf16)
        low = (mixed - high.astype(f32)).astype(bf16)
        both = jnp.dot(
            jnp.concatenate([high, low], axis=0), vu_v[:, k * 128 : (k + 1) * 128],
            preferred_element_type=f32,
        )
        part = both[0:16] + both[16:32]
        part = jnp.where(row == 12, maxima[k : k + 1, :], part)
        part = jnp.where(row == 13, totals[k : k + 1, :], part)
        hb_send[k * 16 : (k + 1) * 16, :] = part

    @each_peer
    def _(peer):
        @pl.when(owns_head(peer))
        def _():
            over_seq(
                HEAD_SUM, rows(hb_send, head_of_owner(peer), 14), rows(hb_recv, me, 14), peer
            ).start()

    own_key = jnp.concatenate([qa_all[(10 + t) * 16 : (11 + t) * 16, :] for t in range(3)], axis=1)
    own_value = jnp.concatenate(
        [qa_all[(12 + t) * 16 : (13 + t) * 16, :] for t in range(3)], axis=1
    ).astype(bf16)
    own = jnp.dot(own_value, vu_v[...], preferred_element_type=f32)
    for k in range(GROUP_HEADS):
        own_v[k * 16 : (k + 1) * 16, :] = own[:, k * 128 : (k + 1) * 128]

    @pl.when(owns_head(me))
    def _():
        k = head_of_owner(me)
        mine = pl.ds(pl.multiple_of(k * 16, 16), 16)
        hb_recv[pl.ds(pl.multiple_of(me * 16, 16), 16), :] = hb_send[mine, :]
        absorbed = jnp.concatenate([absorbed_v[t, mine, :] for t in range(3)], axis=1)
        own_score = jnp.sum(absorbed * own_key, axis=1, keepdims=True) * scaling

        arrived(HEAD_SUM, hb_recv, 15 * 14)

        tops = hb_recv[pl.ds(12, 16, stride=16), :].T[0:16, :]
        sums = hb_recv[pl.ds(13, 16, stride=16), :].T[0:16, :]
        highest = jnp.maximum(jnp.max(tops, axis=1, keepdims=True), own_score)
        shares = jnp.exp(tops - highest)
        own_weight = jnp.exp(own_score - highest)
        denominator = jnp.sum(shares * sums, axis=1, keepdims=True) + own_weight
        total = own_weight * own_v[mine, :]
        for i in range(SEQ):
            total = total + shares[:, i : i + 1] * hb_recv[i * 16 : (i + 1) * 16, :]
        head_out = (total / denominator).astype(bf16).astype(f32)
        hb_all[mine, :] = jnp.where(row < ROWS, head_out, 0.0)

        @each_peer
        def _(peer):
            over_seq(HEAD_ALL, rows(hb_all, k, ROWS), rows(hb_all, k, ROWS), peer).start()

    either(HEAD_ALL, hb_all, owns_head(me), GROUP_HEADS, ROWS, arrived)

    def over_heads(src, dst, peer):
        return pltpu.make_async_remote_copy(
            src_ref=src, dst_ref=dst,
            send_sem=x_send_sem.at[peer], recv_sem=x_recv_sem.at[hme],
            device_id={"heads": peer}, device_id_type=MESH,
        )

    l_wo.wait()
    heads_out = jnp.concatenate(
        [hb_all[k * 16 : (k + 1) * 16, :] for k in range(GROUP_HEADS)], axis=1
    ).astype(bf16)
    attn = lax.dot_general(
        heads_out, wo_v[...], (((1,), (1,)), ((), ())), preferred_element_type=f32
    )
    tile_lane, tile_sub = iota((8, 128), 1), iota((8, 128), 0)
    last = jnp.concatenate([attn[:, 256:320], attn[:, 256:320]], axis=1)
    at_send[:, 0:256] = attn[0:8, 0:256]
    at_send[:, 256:384] = jnp.where(tile_lane < 64, last[0:8], last[8:16])
    at_send[:, 384:512] = jnp.where(
        tile_sub < 4, attn[8:16, 0:128], pltpu.roll(attn[8:16, 128:256], 4, 0)
    )
    for j in range(1, heads_size):
        peer = lax.rem(hme + j, heads_size)
        over_heads(at_send, at_recv.at[hme], peer).start()
    at_recv[hme] = at_send[...]
    l_fgain.wait()
    for j in range(1, heads_size):
        peer = lax.rem(hme + j, heads_size)
        pltpu.make_async_copy(at_send, at_send, x_recv_sem.at[peer]).wait()
    attn = at_recv[0]
    for h in range(1, heads_size):
        attn = attn + at_recv[h]
    upper = attn[:, 0:320]
    low = attn[:, 384:512]
    lower8 = jnp.concatenate(
        [low, pltpu.roll(low, 4, 0), pltpu.roll(attn[:, 256:384], 64, 1)[:, 0:64]], axis=1
    )
    updated = states_v[...] + jnp.concatenate([upper, lower8], axis=0)
    new_hidden[...] = updated[0:ROWS].astype(bf16)
    sq_send[...] = as_row(jnp.sum(updated * updated, axis=1, keepdims=True))

    @each_peer
    def _(peer):
        over_seq(SQUARES, sq_send, sq_recv.at[me], peer).start()

    scaled = updated * fgain_v[...].reshape(1, RANK)
    bottom = scaled[8:16]
    bottom = jnp.where(iota(bottom.shape, 0) < 4, bottom, pltpu.roll(bottom, 4, 0))
    twice = jnp.concatenate([scaled[0:8], bottom], axis=0).astype(bf16)
    l_wv.wait()
    lower = iota((8, 256), 0) < 4

    def piece(c):
        terms = jnp.dot(
            twice, wv_v[:, pl.ds(pl.multiple_of(c * WIDE, WIDE), WIDE)], preferred_element_type=f32
        )
        vd_send[c, :, 0:512] = terms[0:8]
        vd_send[c, :, 512:768] = jnp.where(lower, terms[8:16, 0:256], terms[8:16, 256:512])

    def last_piece():
        terms = jnp.dot(twice, wv_v[:, 15 * WIDE : VOCAB_LOCAL], preferred_element_type=f32)
        vd_send[15] = jnp.zeros((8, 768), f32)
        vd_send[15, :, 0:TAIL] = terms[0:8]
        vd_send[15, 0:4, 512:768] = terms[8:12, 0:256]
        vd_send[15, 4:8, 512 : 512 + TAIL - 256] = terms[12:16, 256:TAIL]

    def any_piece(c):
        @pl.when(c < 15)
        def _():
            piece(c)

        @pl.when(c == 15)
        def _():
            last_piece()

    def at(over_y, over_z):
        return lax.rem(lax.div(me, 8) + over_y, 2) * 8 + lax.rem(lax.rem(me, 8) + over_z, 8)

    def each_side(step):
        @pl.loop(0, 6)
        def _(j):
            t, back = lax.div(j, 2), lax.rem(j, 2)
            step((1 - back) * (3 - t) + back * (5 + t))

    direct = core == 0
    by_half = core == 1

    @pl.when(direct)
    def _():
        @each_peer
        def _(peer):
            any_piece(peer)
            over_seq(VOCAB_SUM, vd_send.at[peer], vd_recv.at[me], peer).start()

    @pl.when(by_half)
    def _():
        @each_side
        def _(over_z):
            any_piece(at(1, over_z))
            pltpu.make_async_remote_copy(
                src_ref=vd_send.at[at(1, over_z)], dst_ref=vd_half.at[over_z],
                send_sem=send_sem.at[VOCAB_HALF], recv_sem=half_sem.at[over_z],
                device_id={"seq": at(1, 0)}, device_id_type=MESH,
            ).start()

        @pl.loop(0, 3)
        def _(j):
            peer = at(1 - lax.rem(j, 2), 4 - 4 * lax.div(j, 2))
            any_piece(peer)
            over_seq(VOCAB_SUM, vd_send.at[peer], vd_recv.at[me], peer).start()

        @each_side
        def _(over_z):
            any_piece(at(0, over_z))

    any_piece(me)
    vd_recv[me] = vd_send[me]
    sq_recv[me] = sq_send[...]
    @pl.when(by_half)
    def _():
        @each_side
        def _(over_z):
            peer = at(0, over_z)
            half = vd_half.at[over_z]
            pltpu.make_async_copy(half, half, half_sem.at[over_z]).wait()
            vd_send[peer] = vd_send[peer] + vd_half[over_z]
            over_seq(VOCAB_SUM, vd_send.at[peer], vd_recv.at[me], peer).start()

    @pl.when(direct)
    def _():
        sent(VOCAB_SUM, vd_send, 15)
        pl.semaphore_signal(turn_sem, inc=1, device_id={"batch": partner}, device_id_type=MESH)

    arrived(SQUARES, sq_recv, 15)
    @pl.when(direct)
    def _():
        arrived(VOCAB_SUM, vd_recv, 15)
        share = vd_recv[0]
        for i in range(1, SEQ):
            share = share + vd_recv[i]
        vd_half[0] = share

    @pl.when(by_half)
    def _():
        arrived(VOCAB_SUM, vd_recv, 9)
        share = vd_recv[me] + vd_recv[at(1, 0)] + vd_recv[at(1, 4)]
        for over_z in range(1, 8):
            share = share + vd_recv[at(0, over_z)]
        vd_half[0] = share

    square_total = sq_recv[0]
    for i in range(1, SEQ):
        square_total = square_total + sq_recv[i]
    share = vd_half[0]
    inv = lax.rsqrt(square_total / D + epsilon)
    sub = iota((8, 128), 0)
    inv_top = as_column(inv, sub)
    inv_bottom = as_column(inv, 8 + lax.rem(sub, 4))
    spot = iota((8, 512), 1)
    spot_bottom = iota((8, 256), 1) + jnp.where(lower, 0, 256)
    limit = VOCAB_LOCAL - me * WIDE
    vd_all[me, :, 0:512] = jnp.where(spot < limit, share[:, 0:512] * inv_top, negative_fill)
    vd_all[me, :, 512:768] = jnp.where(
        spot_bottom < limit, share[:, 512:768] * inv_bottom, negative_fill
    )

    @pl.when(core == 1)
    def _():
        pl.semaphore_wait(turn_sem, 1)

    def send_logits(over_y, over_z):
        over_seq(VOCAB_ALL, vd_all.at[me], vd_all.at[me], at(over_y, over_z)).start()

    def send_near(over_z):
        pltpu.make_async_remote_copy(
            src_ref=vd_all.at[me], dst_ref=vd_all.at[me],
            send_sem=send_sem.at[VOCAB_ALL], recv_sem=near_sem.at[8 - over_z],
            device_id={"seq": at(0, over_z)}, device_id_type=MESH,
        ).start()

    near = [d for t in range(NEAR, 0, -1) for d in (t, 8 - t)]
    far = [d for t in range(3, NEAR, -1) for d in (t, 8 - t)]

    def send_direct(peer):
        over_seq(VOCAB_ALL, vd_all.at[me], vd_all.at[me], peer).start()

    @pl.when(direct)
    def _():
        each_peer(send_direct, 0, 2)

    @pl.when(by_half)
    def _():
        for over_z in near[:2]:
            send_near(over_z)

    l_draft.wait()
    sub1 = iota((8, 1), 0)
    draft_top = jnp.zeros((8, 1), jnp.int32)
    draft_bottom = jnp.zeros((8, 1), jnp.int32)
    for b in range(8):
        draft_top = jnp.where(sub1 == b, draft_s[b], draft_top)
    for b in range(4):
        draft_bottom = jnp.where(lax.rem(sub1, 4) == b, draft_s[8 + b], draft_bottom)
    first = hme * VOCAB_LOCAL + me * WIDE
    draft_top = draft_top - first
    draft_bottom = draft_bottom - first

    def other_half(column):
        return pltpu.roll(jnp.broadcast_to(column, (8, 128)), 4, 0)[:, 0:1]

    high = vd_all[me, :, 0:512]
    low = vd_all[me, :, 512:768]
    max_top = jnp.max(high, axis=1, keepdims=True)
    max_bottom = jnp.max(low, axis=1, keepdims=True)
    max_bottom = jnp.maximum(max_bottom, other_half(max_bottom))
    sum_top = jnp.sum(jnp.exp(high - max_top), axis=1, keepdims=True)
    sum_bottom = jnp.sum(jnp.exp(low - max_bottom), axis=1, keepdims=True)
    sum_bottom = sum_bottom + other_half(sum_bottom)
    pick_top = jnp.sum(
        jnp.where((spot == draft_top) & (spot < limit), high, 0.0), axis=1, keepdims=True
    )
    pick_bottom = jnp.sum(
        jnp.where((spot_bottom == draft_bottom) & (spot_bottom < limit), low, 0.0),
        axis=1, keepdims=True,
    )
    pick_bottom = pick_bottom + other_half(pick_bottom)

    lane8 = iota((8, 128), 1)
    block = jnp.zeros((8, 128), f32)
    for i, (upper, under) in enumerate(
        ((max_top, max_bottom), (sum_top, sum_bottom), (pick_top, pick_bottom))
    ):
        block = jnp.where(lane8 == sub + 16 * i, upper, block)
        block = jnp.where((lane8 == sub + 16 * i + 8) & (sub < 4), under, block)
    stats = jnp.sum(block, axis=0, keepdims=True)
    st_send[...] = stats
    slot = hme * SEQ + me
    st_recv[slot] = stats

    def send_stats(peer, j):
        pltpu.make_async_remote_copy(
            src_ref=st_send, dst_ref=st_recv.at[slot],
            send_sem=send_sem.at[STATS], recv_sem=recv_sem.at[STATS],
            device_id={"seq": peer, "heads": lax.rem(hme + j, heads_size)}, device_id_type=MESH,
        ).start()

    @each_peer
    def _(peer):
        for j in range(heads_size):
            send_stats(peer, j)

    for j in range(1, heads_size):
        send_stats(me, j)

    @pl.when(direct)
    def _():
        each_peer(send_direct, 2, SEQ - 1)

    @pl.when(by_half)
    def _():
        send_logits(1, 4)
        for over_z in far:
            send_logits(1, over_z)
        for over_z in near[2:]:
            send_near(over_z)
        send_logits(0, 4)
        for over_z in far:
            send_logits(0, over_z)
        send_logits(1, 0)
        for over_z in near[::-1]:
            there = vd_all.at[at(0, over_z)]
            pltpu.make_async_copy(there, there, near_sem.at[over_z]).wait()
            over_seq(VOCAB_ALL, there, there, at(1, 0)).start()

    either(QUERY_SUM, qa_send, me < PIECES, PIECES, 13, sent)

    @pl.when(me < PIECES)
    def _():
        sent(QUERY_ALL, qa_recv, 15 * ROWS)

    either(HEAD_SUM, hb_send, owns_head(me), GROUP_HEADS, 14, sent)

    @pl.when(owns_head(me))
    def _():
        sent(HEAD_ALL, hb_recv, 15 * ROWS)

    sent(SQUARES, sq_recv, 15)

    @pl.when(by_half)
    def _():
        sent(VOCAB_SUM, vd_send, 9)
        sent(VOCAB_HALF, vd_send, 6)

    for j in range(1, heads_size):
        peer = lax.rem(hme + j, heads_size)
        pltpu.make_async_copy(at_send, at_send, x_send_sem.at[peer]).wait()

    @pl.when(direct)
    def _():
        arrived(VOCAB_ALL, vd_all, 15)

    @pl.when(by_half)
    def _():
        arrived(VOCAB_ALL, vd_all, 15 - 2 * NEAR)

    arrived(STATS, st_recv, heads_size * SEQ - 1)
    every = [st_recv[i] for i in range(heads_size * SEQ)]
    highest = functools.reduce(jnp.maximum, every)
    total = jnp.zeros((1, 128), f32)
    picked = jnp.zeros((1, 128), f32)
    for one in every:
        total = total + jnp.exp(one - highest) * pltpu.roll(one, 112, 1)
        picked = picked + one
    log_total = highest + jnp.log(jnp.where(lane8[0:1] < ROWS, total, 1.0))
    draft_out[...] = pltpu.roll(picked, 96, 1) - log_total
    log_top = as_column(log_total, sub)
    log_bottom = as_column(log_total, 8 + lax.rem(sub, 4))
    logs_out[...] = jnp.where(lane8 == 0, log_top, log_bottom)
    sent(VOCAB_ALL, vd_recv, 15)
    sent(STATS, st_recv, heads_size * SEQ - 1)


def closing_kernel(
    new_hidden, logits, logs, draft, hidden_out, probs_out, draft_out, upper_v, lower_v, draft_v, sem
):
    copies = [
        pltpu.make_async_copy(new_hidden, hidden_out, sem.at[0]),
        pltpu.make_async_copy(draft_v, draft_out, sem.at[1]),
        pltpu.make_async_copy(upper_v, probs_out.at[pl.ds(0, 8)], sem.at[2]),
        pltpu.make_async_copy(lower_v, probs_out.at[pl.ds(8, 4)], sem.at[3]),
    ]
    copies[0].start()
    draft_v[...] = draft[...].reshape(128)[:ROWS]
    copies[1].start()
    log_top, log_bottom = logs[:, 0:1], logs[:, 1:2]
    for c in range(SEQ):
        at = c * WIDE
        width = min(WIDE, VOCAB_LOCAL - at)
        upper_v[:, at : at + width] = logits[c, :, 0:width] - log_top
    copies[2].start()
    for c in range(SEQ):
        at = c * WIDE
        low = logits[c, :, 512:768] - log_bottom
        lower_v[:, at : at + 256] = low[0:4]
        rest = min(256, VOCAB_LOCAL - at - 256)
        lower_v[:, at + 256 : at + 256 + rest] = pltpu.roll(low, 4, 0)[0:4, 0:rest]
    copies[3].start()
    for copy in copies:
        copy.wait()


def solution(mesh):
    heads_size = mesh.shape["heads"]

    def body(hidden, lengths, drafts, gain, wq, wl, cache, ku, vu, wo, fgain, wv):
        hbm = pl.BlockSpec(memory_space=pltpu.HBM)
        vmem = pl.BlockSpec(memory_space=pltpu.VMEM)
        width = GROUP_HEADS * HEAD_DIM
        results = pl.pallas_call(
            functools.partial(kernel, heads_size),
            name="decode_step",
            out_shape=(
                jax.ShapeDtypeStruct((ROWS, RANK), bf16),
                jax.ShapeDtypeStruct((SEQ, 8, 768), f32),
                jax.ShapeDtypeStruct((8, 128), f32),
                jax.ShapeDtypeStruct((1, 128), f32),
            ),
            in_specs=[hbm] * 12,
            out_specs=(vmem,) * 4,
            scratch_shapes=[
                pltpu.VMEM((ROWS, RANK), bf16),
                pltpu.SMEM((ROWS,), jnp.int32),
                pltpu.SMEM((ROWS,), jnp.int32),
                pltpu.VMEM((RANK,), f32),
                pltpu.VMEM((RANK, width), bf16),
                pltpu.VMEM((RANK, 2 * RANK), bf16),
                pltpu.VMEM((ROWS, SPAN, 2 * RANK), bf16),
                pltpu.VMEM((RANK, width), bf16),
                pltpu.VMEM((384, width), bf16),
                pltpu.VMEM((RANK, width), bf16),
                pltpu.VMEM((RANK,), f32),
                pltpu.VMEM((RANK, VOCAB_LOCAL), bf16),
                pltpu.VMEM((16, RANK), f32),
                pltpu.VMEM((256, 128), f32),
                pltpu.VMEM((256, 128), f32),
                pltpu.VMEM((256, 128), f32),
                pltpu.VMEM((3, 256, 128), f32),
                pltpu.VMEM((3, 256, 128), f32),
                pltpu.VMEM((160, 128), f32),
                pltpu.VMEM((256, 128), f32),
                pltpu.VMEM((160, 128), f32),
                pltpu.VMEM((160, 128), f32),
                pltpu.VMEM((8, 512), f32),
                pltpu.VMEM((heads_size, 8, 512), f32),
                pltpu.VMEM((1, 128), f32),
                pltpu.VMEM((SEQ, 1, 128), f32),
                pltpu.VMEM((SEQ, 8, 768), f32),
                pltpu.VMEM((SEQ, 8, 768), f32),
                pltpu.VMEM((8, 8, 768), f32),
                pltpu.VMEM((1, 128), f32),
                pltpu.VMEM((heads_size * SEQ, 1, 128), f32),
                pltpu.SemaphoreType.DMA((12,)),
                pltpu.SemaphoreType.DMA((9,)),
                pltpu.SemaphoreType.DMA((9,)),
                pltpu.SemaphoreType.DMA((heads_size,)),
                pltpu.SemaphoreType.DMA((heads_size,)),
                pltpu.SemaphoreType.REGULAR,
                pltpu.SemaphoreType.DMA((8,)),
                pltpu.SemaphoreType.DMA((8,)),
            ],
            compiler_params=pltpu.CompilerParams(
                collective_id=0, has_side_effects=True, vmem_limit_bytes=48 * 1024 * 1024
            ),
        )(*(pltpu.with_memory_space_constraint(x, pltpu.HBM) for x in (
            hidden, lengths, drafts, gain, wq, wl.reshape(RANK, 2 * RANK),
            cache.reshape(ROWS, SPAN, 2 * RANK), ku.reshape(RANK, width), vu.reshape(RANK, width),
            wo.T, fgain, wv,
        )))
        return pl.pallas_call(
            closing_kernel,
            name="outputs",
            out_shape=(
                jax.ShapeDtypeStruct((ROWS, RANK), bf16),
                jax.ShapeDtypeStruct((ROWS, VOCAB_LOCAL), f32),
                jax.ShapeDtypeStruct((ROWS,), f32),
            ),
            in_specs=[vmem] * 4,
            out_specs=(hbm,) * 3,
            scratch_shapes=[
                pltpu.VMEM((8, VOCAB_LOCAL), f32),
                pltpu.VMEM((4, VOCAB_LOCAL), f32),
                pltpu.VMEM((ROWS,), f32),
                pltpu.SemaphoreType.DMA((4,)),
            ],
            compiler_params=pltpu.CompilerParams(vmem_limit_bytes=4 * 1024 * 1024),
        )(*results)

    return jax.shard_map(
        body,
        mesh=mesh,
        in_specs=(
            P("batch", "seq"), P("batch"), P("batch"), P("seq"), P("seq", "heads"),
            P("seq", "heads", None), P("batch", "heads", "seq", None), P("heads", None, None),
            P("heads", None, None), P("heads", "seq"), P("seq"), P("seq", "heads"),
        ),
        out_specs=(P("batch", "seq"), P("batch", "heads"), P("batch")),
        check_vma=False,
    )
```

```python
import functools
import math

import jax
import jax.numpy as jnp
from jax import lax
from jax.experimental import pallas as pl
from jax.experimental.pallas import tpu as pltpu
from jax.sharding import PartitionSpec as P

D = 5120
HEAD_DIM = 128
GROUP_HEADS = 10
RANK = 320
SEQ = 16
ROWS = 12
SPAN = 256
WIDE = 512
VOCAB_LOCAL = 8000
PIECES = 15
NEAR = 2
TAIL = VOCAB_LOCAL - 15 * WIDE

MESH = pl.DeviceIdType.MESH
f32 = jnp.float32
bf16 = jnp.bfloat16
epsilon = 1e-05
negative_fill = -1e30
scaling = 1.0 / math.sqrt(HEAD_DIM)

QUERY_SUM, QUERY_ALL, HEAD_SUM, HEAD_ALL, SQUARES, VOCAB_SUM, VOCAB_ALL, STATS, VOCAB_HALF = range(9)


def owner_of_head(k):
    return lax.div(k * 8, 5)


def head_of_owner(s):
    return lax.div(s * 5 + 7, 8)


def owns_head(s):
    return owner_of_head(head_of_owner(s)) == s


def iota(shape, dim):
    return lax.broadcasted_iota(jnp.int32, shape, dim)


def as_row(column):
    spread = jnp.where(iota((16, 128), 0) == iota((16, 128), 1), column, 0.0)
    return jnp.sum(spread, axis=0, keepdims=True)


def as_column(row, picks):
    return jnp.sum(jnp.where(picks == iota(picks.shape, 1), row, 0.0), axis=1, keepdims=True)


def kernel(
    heads_size,
    hidden, lengths, drafts, gain, wq, wl, cache, ku, vu, wo, fgain, wv,
    new_hidden, vd_all, logs_out, draft_out,
    hid_v, len_s, draft_s, gain_v, wq_v, wl_v, cache_v, ku_v, vu_v, wo_v, fgain_v, wv_v,
    states_v,
    qa_send, qa_recv, qa_all,
    absorbed_v, mixed_v,
    hb_send, hb_recv, hb_all, own_v,
    at_send, at_recv,
    sq_send, sq_recv,
    vd_send, vd_recv, vd_half,
    st_send, st_recv,
    load_sem, send_sem, recv_sem, x_send_sem, x_recv_sem, turn_sem, near_sem, half_sem,
):
    me = lax.axis_index("seq")
    hme = lax.axis_index("heads")
    batch = lax.axis_index("batch")
    core = lax.rem(batch, 2)
    partner = batch + 1 - 2 * core

    def peer_at(j):
        t = lax.div(j, 2)
        over_z = 4 + (1 - 2 * lax.rem(t, 2)) * lax.div(t + 1, 2)
        y, z = lax.div(me, 8), lax.rem(me, 8)
        return lax.rem(y + 1 - lax.rem(j, 2), 2) * 8 + lax.rem(z + over_z, 8)

    def each_peer(step, start=0, stop=SEQ - 1):
        @pl.loop(start, stop)
        def _(j):
            step(peer_at(j))

    barrier = pltpu.get_barrier_semaphore()

    @each_peer
    def _(peer):
        pl.semaphore_signal(barrier, inc=1, device_id={"seq": peer}, device_id_type=MESH)

    pl.semaphore_signal(barrier, inc=1, device_id={"batch": partner}, device_id_type=MESH)
    for j in range(1, heads_size):
        pl.semaphore_signal(
            barrier, inc=1, device_id={"heads": lax.rem(hme + j, heads_size)}, device_id_type=MESH
        )

    loads = [
        (hidden, hid_v), (gain, gain_v), (lengths, len_s), (drafts, draft_s), (fgain, fgain_v),
        (wq, wq_v), (wl, wl_v), (ku, ku_v), (cache, cache_v), (vu, vu_v.at[pl.ds(64, RANK)]),
        (wo, wo_v), (wv, wv_v),
    ]
    loads = [pltpu.make_async_copy(a, b, load_sem.at[i]) for i, (a, b) in enumerate(loads)]
    l_hid, l_gain, l_len, l_draft, l_fgain, l_wq, l_wl, l_ku, l_cache, l_vu, l_wo, l_wv = loads
    for load in loads:
        load.start()

    def over_seq(phase, src, dst, peer):
        return pltpu.make_async_remote_copy(
            src_ref=src, dst_ref=dst,
            send_sem=send_sem.at[phase], recv_sem=recv_sem.at[phase],
            device_id={"seq": peer}, device_id_type=MESH,
        )

    def arrived(phase, ref, count):
        ref = ref.at[pl.ds(0, count)]
        pltpu.make_async_copy(ref, ref, recv_sem.at[phase]).wait()

    def sent(phase, ref, count):
        ref = ref.at[pl.ds(0, count)]
        pltpu.make_async_copy(ref, ref, send_sem.at[phase]).wait()

    def rows(ref, i, count):
        return ref.at[pl.ds(pl.multiple_of(i * 16, 16), count)]

    def either(phase, ref, condition, count, size, waits):
        @pl.when(condition)
        def _():
            waits(phase, ref, (count - 1) * size)

        @pl.when(jnp.logical_not(condition))
        def _():
            waits(phase, ref, count * size)

    vu_v[0:64, :] = jnp.zeros((64, GROUP_HEADS * HEAD_DIM), bf16)
    absorbed_v[...] = jnp.zeros_like(absorbed_v)
    mixed_v[...] = jnp.zeros_like(mixed_v)
    states_v[...] = jnp.zeros_like(states_v)
    l_hid.wait()
    l_gain.wait()
    states_v[0:ROWS, :] = hid_v[...].astype(f32)
    states = states_v[...]
    gained = (states * gain_v[...].reshape(1, RANK)).astype(bf16)
    squares = as_row(jnp.sum(states * states, axis=1, keepdims=True))
    row = iota((16, 128), 0)
    l_wq.wait()
    query_part = jnp.dot(gained, wq_v[...], preferred_element_type=f32)
    for k in range(10):
        part = query_part[:, k * 128 : (k + 1) * 128]
        qa_send[k * 16 : (k + 1) * 16, :] = jnp.where(row == 12, squares, part)
    l_wl.wait()
    latent_part = jnp.dot(gained, wl_v[...], preferred_element_type=f32)
    for k in range(5):
        part = latent_part[:, k * 128 : (k + 1) * 128]
        qa_send[(k + 10) * 16 : (k + 11) * 16, :] = jnp.where(row == 12, squares, part)

    pl.semaphore_wait(barrier, SEQ + heads_size - 1)

    @each_peer
    def _(peer):
        @pl.when(peer < PIECES)
        def _():
            over_seq(QUERY_SUM, rows(qa_send, peer, 13), rows(qa_recv, me, 13), peer).start()

    @pl.when(me < PIECES)
    def _():
        qa_recv[pl.ds(pl.multiple_of(me * 16, 16), 16), :] = qa_send[
            pl.ds(pl.multiple_of(me * 16, 16), 16), :
        ]

        arrived(QUERY_SUM, qa_recv, 15 * 13)

        total = qa_recv[0:16, :]
        for i in range(1, SEQ):
            total = total + qa_recv[i * 16 : (i + 1) * 16, :]
        mean = as_column(total[12:13, :], row) / D
        done = (lax.rsqrt(mean + epsilon) * total).astype(bf16).astype(f32)
        qa_all[pl.ds(pl.multiple_of(me * 16, 16), 16), :] = jnp.where(row < ROWS, done, 0.0)

        @each_peer
        def _(peer):
            over_seq(QUERY_ALL, rows(qa_all, me, ROWS), rows(qa_all, me, ROWS), peer).start()

    either(QUERY_ALL, qa_all, me < PIECES, PIECES, ROWS, arrived)

    l_ku.wait()
    for k in range(GROUP_HEADS):
        query = qa_all[k * 16 : (k + 1) * 16, :].astype(bf16)
        absorbed = lax.dot_general(
            query, ku_v[:, k * 128 : (k + 1) * 128], (((1,), (1,)), ((), ())),
            preferred_element_type=f32,
        )
        absorbed = absorbed.astype(bf16).astype(f32)
        absorbed_v[0, k * 16 : (k + 1) * 16, :] = absorbed[:, 0:128]
        absorbed_v[1, k * 16 : (k + 1) * 16, :] = absorbed[:, 128:256]
        absorbed_v[2, k * 16 : (k + 1) * 16, 0:64] = absorbed[:, 256:320]

    l_len.wait()
    l_cache.wait()
    positions = me * SPAN + iota((16, SPAN), 1)
    lane = iota((16, 128), 1)
    maxima = jnp.zeros((16, 128), f32)
    totals = jnp.zeros((16, 128), f32)
    scores = []
    for b in range(ROWS):
        one = jnp.concatenate(
            [absorbed_v[t, pl.ds(b, 16, stride=16), :] for t in range(3)], axis=1
        ).astype(bf16)
        scores.append(
            lax.dot_general(
                one, cache_v[b, :, 0:384], (((1,), (1,)), ((), ())), preferred_element_type=f32
            )
        )
    weights = []
    for b in range(ROWS):
        live = positions < len_s[b]
        score = jnp.where(live, scores[b] * scaling, negative_fill)
        top = jnp.max(score, axis=1, keepdims=True)
        weight = jnp.where(live, jnp.exp(score - top), 0.0)
        maxima = jnp.where(lane == b, top, maxima)
        totals = jnp.where(lane == b, jnp.sum(weight, axis=1, keepdims=True), totals)
        weights.append(weight.astype(bf16))
    for b in range(ROWS):
        mixed = jnp.dot(weights[b], cache_v[b, :, 256:640], preferred_element_type=f32)
        for t in range(3):
            mixed_v[t, b * 16 : (b + 1) * 16, :] = mixed[:, t * 128 : (t + 1) * 128]

    l_vu.wait()
    for k in range(GROUP_HEADS):
        mixed = jnp.concatenate(
            [mixed_v[t, pl.ds(k, 16, stride=16), :] for t in range(3)], axis=1
        )
        high = mixed.astype(bf16)
        low = (mixed - high.astype(f32)).astype(bf16)
        both = jnp.dot(
            jnp.concatenate([high, low], axis=0), vu_v[:, k * 128 : (k + 1) * 128],
            preferred_element_type=f32,
        )
        part = both[0:16] + both[16:32]
        part = jnp.where(row == 12, maxima[k : k + 1, :], part)
        part = jnp.where(row == 13, totals[k : k + 1, :], part)
        hb_send[k * 16 : (k + 1) * 16, :] = part

    @each_peer
    def _(peer):
        @pl.when(owns_head(peer))
        def _():
            over_seq(
                HEAD_SUM, rows(hb_send, head_of_owner(peer), 14), rows(hb_recv, me, 14), peer
            ).start()

    own_key = jnp.concatenate([qa_all[(10 + t) * 16 : (11 + t) * 16, :] for t in range(3)], axis=1)
    own_value = jnp.concatenate(
        [qa_all[(12 + t) * 16 : (13 + t) * 16, :] for t in range(3)], axis=1
    ).astype(bf16)
    own = jnp.dot(own_value, vu_v[...], preferred_element_type=f32)
    for k in range(GROUP_HEADS):
        own_v[k * 16 : (k + 1) * 16, :] = own[:, k * 128 : (k + 1) * 128]

    @pl.when(owns_head(me))
    def _():
        k = head_of_owner(me)
        mine = pl.ds(pl.multiple_of(k * 16, 16), 16)
        hb_recv[pl.ds(pl.multiple_of(me * 16, 16), 16), :] = hb_send[mine, :]
        absorbed = jnp.concatenate([absorbed_v[t, mine, :] for t in range(3)], axis=1)
        own_score = jnp.sum(absorbed * own_key, axis=1, keepdims=True) * scaling

        arrived(HEAD_SUM, hb_recv, 15 * 14)

        tops = hb_recv[pl.ds(12, 16, stride=16), :].T[0:16, :]
        sums = hb_recv[pl.ds(13, 16, stride=16), :].T[0:16, :]
        highest = jnp.maximum(jnp.max(tops, axis=1, keepdims=True), own_score)
        shares = jnp.exp(tops - highest)
        own_weight = jnp.exp(own_score - highest)
        denominator = jnp.sum(shares * sums, axis=1, keepdims=True) + own_weight
        total = own_weight * own_v[mine, :]
        for i in range(SEQ):
            total = total + shares[:, i : i + 1] * hb_recv[i * 16 : (i + 1) * 16, :]
        head_out = (total / denominator).astype(bf16).astype(f32)
        hb_all[mine, :] = jnp.where(row < ROWS, head_out, 0.0)

        @each_peer
        def _(peer):
            over_seq(HEAD_ALL, rows(hb_all, k, ROWS), rows(hb_all, k, ROWS), peer).start()

    either(HEAD_ALL, hb_all, owns_head(me), GROUP_HEADS, ROWS, arrived)

    def over_heads(src, dst, peer):
        return pltpu.make_async_remote_copy(
            src_ref=src, dst_ref=dst,
            send_sem=x_send_sem.at[peer], recv_sem=x_recv_sem.at[hme],
            device_id={"heads": peer}, device_id_type=MESH,
        )

    l_wo.wait()
    heads_out = jnp.concatenate(
        [hb_all[k * 16 : (k + 1) * 16, :] for k in range(GROUP_HEADS)], axis=1
    ).astype(bf16)
    attn = lax.dot_general(
        heads_out, wo_v[...], (((1,), (1,)), ((), ())), preferred_element_type=f32
    )
    tile_lane, tile_sub = iota((8, 128), 1), iota((8, 128), 0)
    last = jnp.concatenate([attn[:, 256:320], attn[:, 256:320]], axis=1)
    at_send[:, 0:256] = attn[0:8, 0:256]
    at_send[:, 256:384] = jnp.where(tile_lane < 64, last[0:8], last[8:16])
    at_send[:, 384:512] = jnp.where(
        tile_sub < 4, attn[8:16, 0:128], pltpu.roll(attn[8:16, 128:256], 4, 0)
    )
    for j in range(1, heads_size):
        peer = lax.rem(hme + j, heads_size)
        over_heads(at_send, at_recv.at[hme], peer).start()
    at_recv[hme] = at_send[...]
    l_fgain.wait()
    for j in range(1, heads_size):
        peer = lax.rem(hme + j, heads_size)
        pltpu.make_async_copy(at_send, at_send, x_recv_sem.at[peer]).wait()
    attn = at_recv[0]
    for h in range(1, heads_size):
        attn = attn + at_recv[h]
    upper = attn[:, 0:320]
    low = attn[:, 384:512]
    lower8 = jnp.concatenate(
        [low, pltpu.roll(low, 4, 0), pltpu.roll(attn[:, 256:384], 64, 1)[:, 0:64]], axis=1
    )
    updated = states_v[...] + jnp.concatenate([upper, lower8], axis=0)
    new_hidden[...] = updated[0:ROWS].astype(bf16)
    sq_send[...] = as_row(jnp.sum(updated * updated, axis=1, keepdims=True))

    @each_peer
    def _(peer):
        over_seq(SQUARES, sq_send, sq_recv.at[me], peer).start()

    scaled = updated * fgain_v[...].reshape(1, RANK)
    bottom = scaled[8:16]
    bottom = jnp.where(iota(bottom.shape, 0) < 4, bottom, pltpu.roll(bottom, 4, 0))
    twice = jnp.concatenate([scaled[0:8], bottom], axis=0).astype(bf16)
    l_wv.wait()
    lower = iota((8, 256), 0) < 4

    def piece(c):
        terms = jnp.dot(
            twice, wv_v[:, pl.ds(pl.multiple_of(c * WIDE, WIDE), WIDE)], preferred_element_type=f32
        )
        vd_send[c, :, 0:512] = terms[0:8]
        vd_send[c, :, 512:768] = jnp.where(lower, terms[8:16, 0:256], terms[8:16, 256:512])

    def last_piece():
        terms = jnp.dot(twice, wv_v[:, 15 * WIDE : VOCAB_LOCAL], preferred_element_type=f32)
        vd_send[15] = jnp.zeros((8, 768), f32)
        vd_send[15, :, 0:TAIL] = terms[0:8]
        vd_send[15, 0:4, 512:768] = terms[8:12, 0:256]
        vd_send[15, 4:8, 512 : 512 + TAIL - 256] = terms[12:16, 256:TAIL]

    def any_piece(c):
        @pl.when(c < 15)
        def _():
            piece(c)

        @pl.when(c == 15)
        def _():
            last_piece()

    def at(over_y, over_z):
        return lax.rem(lax.div(me, 8) + over_y, 2) * 8 + lax.rem(lax.rem(me, 8) + over_z, 8)

    def each_side(step):
        @pl.loop(0, 6)
        def _(j):
            t, back = lax.div(j, 2), lax.rem(j, 2)
            step((1 - back) * (3 - t) + back * (5 + t))

    direct = core == 0
    by_half = core == 1

    @pl.when(direct)
    def _():
        @each_peer
        def _(peer):
            any_piece(peer)
            over_seq(VOCAB_SUM, vd_send.at[peer], vd_recv.at[me], peer).start()

    @pl.when(by_half)
    def _():
        @each_side
        def _(over_z):
            any_piece(at(1, over_z))
            pltpu.make_async_remote_copy(
                src_ref=vd_send.at[at(1, over_z)], dst_ref=vd_half.at[over_z],
                send_sem=send_sem.at[VOCAB_HALF], recv_sem=half_sem.at[over_z],
                device_id={"seq": at(1, 0)}, device_id_type=MESH,
            ).start()

        @pl.loop(0, 3)
        def _(j):
            peer = at(1 - lax.rem(j, 2), 4 - 4 * lax.div(j, 2))
            any_piece(peer)
            over_seq(VOCAB_SUM, vd_send.at[peer], vd_recv.at[me], peer).start()

        @each_side
        def _(over_z):
            any_piece(at(0, over_z))

    any_piece(me)
    vd_recv[me] = vd_send[me]
    sq_recv[me] = sq_send[...]
    @pl.when(by_half)
    def _():
        @each_side
        def _(over_z):
            peer = at(0, over_z)
            half = vd_half.at[over_z]
            pltpu.make_async_copy(half, half, half_sem.at[over_z]).wait()
            vd_send[peer] = vd_send[peer] + vd_half[over_z]
            over_seq(VOCAB_SUM, vd_send.at[peer], vd_recv.at[me], peer).start()

    @pl.when(direct)
    def _():
        sent(VOCAB_SUM, vd_send, 15)
        pl.semaphore_signal(turn_sem, inc=1, device_id={"batch": partner}, device_id_type=MESH)

    arrived(SQUARES, sq_recv, 15)
    @pl.when(direct)
    def _():
        arrived(VOCAB_SUM, vd_recv, 15)
        share = vd_recv[0]
        for i in range(1, SEQ):
            share = share + vd_recv[i]
        vd_half[0] = share

    @pl.when(by_half)
    def _():
        arrived(VOCAB_SUM, vd_recv, 9)
        share = vd_recv[me] + vd_recv[at(1, 0)] + vd_recv[at(1, 4)]
        for over_z in range(1, 8):
            share = share + vd_recv[at(0, over_z)]
        vd_half[0] = share

    square_total = sq_recv[0]
    for i in range(1, SEQ):
        square_total = square_total + sq_recv[i]
    share = vd_half[0]
    inv = lax.rsqrt(square_total / D + epsilon)
    sub = iota((8, 128), 0)
    inv_top = as_column(inv, sub)
    inv_bottom = as_column(inv, 8 + lax.rem(sub, 4))
    spot = iota((8, 512), 1)
    spot_bottom = iota((8, 256), 1) + jnp.where(lower, 0, 256)
    limit = VOCAB_LOCAL - me * WIDE
    vd_all[me, :, 0:512] = jnp.where(spot < limit, share[:, 0:512] * inv_top, negative_fill)
    vd_all[me, :, 512:768] = jnp.where(
        spot_bottom < limit, share[:, 512:768] * inv_bottom, negative_fill
    )

    @pl.when(core == 1)
    def _():
        pl.semaphore_wait(turn_sem, 1)

    def send_logits(over_y, over_z):
        over_seq(VOCAB_ALL, vd_all.at[me], vd_all.at[me], at(over_y, over_z)).start()

    def send_near(over_z):
        pltpu.make_async_remote_copy(
            src_ref=vd_all.at[me], dst_ref=vd_all.at[me],
            send_sem=send_sem.at[VOCAB_ALL], recv_sem=near_sem.at[8 - over_z],
            device_id={"seq": at(0, over_z)}, device_id_type=MESH,
        ).start()

    near = [d for t in range(NEAR, 0, -1) for d in (t, 8 - t)]
    far = [d for t in range(3, NEAR, -1) for d in (t, 8 - t)]

    def send_direct(peer):
        over_seq(VOCAB_ALL, vd_all.at[me], vd_all.at[me], peer).start()

    @pl.when(direct)
    def _():
        each_peer(send_direct, 0, 2)

    @pl.when(by_half)
    def _():
        for over_z in near[:2]:
            send_near(over_z)

    l_draft.wait()
    sub1 = iota((8, 1), 0)
    draft_top = jnp.zeros((8, 1), jnp.int32)
    draft_bottom = jnp.zeros((8, 1), jnp.int32)
    for b in range(8):
        draft_top = jnp.where(sub1 == b, draft_s[b], draft_top)
    for b in range(4):
        draft_bottom = jnp.where(lax.rem(sub1, 4) == b, draft_s[8 + b], draft_bottom)
    first = hme * VOCAB_LOCAL + me * WIDE
    draft_top = draft_top - first
    draft_bottom = draft_bottom - first

    def other_half(column):
        return pltpu.roll(jnp.broadcast_to(column, (8, 128)), 4, 0)[:, 0:1]

    high = vd_all[me, :, 0:512]
    low = vd_all[me, :, 512:768]
    max_top = jnp.max(high, axis=1, keepdims=True)
    max_bottom = jnp.max(low, axis=1, keepdims=True)
    max_bottom = jnp.maximum(max_bottom, other_half(max_bottom))
    sum_top = jnp.sum(jnp.exp(high - max_top), axis=1, keepdims=True)
    sum_bottom = jnp.sum(jnp.exp(low - max_bottom), axis=1, keepdims=True)
    sum_bottom = sum_bottom + other_half(sum_bottom)
    pick_top = jnp.sum(
        jnp.where((spot == draft_top) & (spot < limit), high, 0.0), axis=1, keepdims=True
    )
    pick_bottom = jnp.sum(
        jnp.where((spot_bottom == draft_bottom) & (spot_bottom < limit), low, 0.0),
        axis=1, keepdims=True,
    )
    pick_bottom = pick_bottom + other_half(pick_bottom)

    lane8 = iota((8, 128), 1)
    block = jnp.zeros((8, 128), f32)
    for i, (upper, under) in enumerate(
        ((max_top, max_bottom), (sum_top, sum_bottom), (pick_top, pick_bottom))
    ):
        block = jnp.where(lane8 == sub + 16 * i, upper, block)
        block = jnp.where((lane8 == sub + 16 * i + 8) & (sub < 4), under, block)
    stats = jnp.sum(block, axis=0, keepdims=True)
    st_send[...] = stats
    slot = hme * SEQ + me
    st_recv[slot] = stats

    def send_stats(peer, j):
        pltpu.make_async_remote_copy(
            src_ref=st_send, dst_ref=st_recv.at[slot],
            send_sem=send_sem.at[STATS], recv_sem=recv_sem.at[STATS],
            device_id={"seq": peer, "heads": lax.rem(hme + j, heads_size)}, device_id_type=MESH,
        ).start()

    for i in range(SEQ - 1):
        peer = peer_at(i)
        for j in range(heads_size):
            send_stats(peer, j)

    for j in range(1, heads_size):
        send_stats(me, j)

    @pl.when(direct)
    def _():
        each_peer(send_direct, 2, SEQ - 1)

    @pl.when(by_half)
    def _():
        send_logits(1, 4)
        for over_z in far:
            send_logits(1, over_z)
        for over_z in near[2:]:
            send_near(over_z)
        send_logits(0, 4)
        for over_z in far:
            send_logits(0, over_z)
        send_logits(1, 0)
        for over_z in near[::-1]:
            there = vd_all.at[at(0, over_z)]
            pltpu.make_async_copy(there, there, near_sem.at[over_z]).wait()
            over_seq(VOCAB_ALL, there, there, at(1, 0)).start()

    either(QUERY_SUM, qa_send, me < PIECES, PIECES, 13, sent)

    @pl.when(me < PIECES)
    def _():
        sent(QUERY_ALL, qa_recv, 15 * ROWS)

    either(HEAD_SUM, hb_send, owns_head(me), GROUP_HEADS, 14, sent)

    @pl.when(owns_head(me))
    def _():
        sent(HEAD_ALL, hb_recv, 15 * ROWS)

    sent(SQUARES, sq_recv, 15)

    @pl.when(by_half)
    def _():
        sent(VOCAB_SUM, vd_send, 9)
        sent(VOCAB_HALF, vd_send, 6)

    for j in range(1, heads_size):
        peer = lax.rem(hme + j, heads_size)
        pltpu.make_async_copy(at_send, at_send, x_send_sem.at[peer]).wait()

    @pl.when(direct)
    def _():
        arrived(VOCAB_ALL, vd_all, 15)

    @pl.when(by_half)
    def _():
        arrived(VOCAB_ALL, vd_all, 15 - 2 * NEAR)

    arrived(STATS, st_recv, heads_size * SEQ - 1)
    every = [st_recv[i] for i in range(heads_size * SEQ)]
    highest = functools.reduce(jnp.maximum, every)
    total = jnp.zeros((1, 128), f32)
    picked = jnp.zeros((1, 128), f32)
    for one in every:
        total = total + jnp.exp(one - highest) * pltpu.roll(one, 112, 1)
        picked = picked + one
    log_total = highest + jnp.log(jnp.where(lane8[0:1] < ROWS, total, 1.0))
    draft_out[...] = pltpu.roll(picked, 96, 1) - log_total
    log_top = as_column(log_total, sub)
    log_bottom = as_column(log_total, 8 + lax.rem(sub, 4))
    logs_out[...] = jnp.where(lane8 == 0, log_top, log_bottom)
    sent(VOCAB_ALL, vd_recv, 15)
    sent(STATS, st_recv, heads_size * SEQ - 1)


def closing_kernel(
    new_hidden, logits, logs, draft, hidden_out, probs_out, draft_out, upper_v, lower_v, draft_v, sem
):
    copies = [
        pltpu.make_async_copy(new_hidden, hidden_out, sem.at[0]),
        pltpu.make_async_copy(draft_v, draft_out, sem.at[1]),
        pltpu.make_async_copy(upper_v, probs_out.at[pl.ds(0, 8)], sem.at[2]),
        pltpu.make_async_copy(lower_v, probs_out.at[pl.ds(8, 4)], sem.at[3]),
    ]
    copies[0].start()
    draft_v[...] = draft[...].reshape(128)[:ROWS]
    copies[1].start()
    log_top, log_bottom = logs[:, 0:1], logs[:, 1:2]
    for c in range(SEQ):
        at = c * WIDE
        width = min(WIDE, VOCAB_LOCAL - at)
        upper_v[:, at : at + width] = logits[c, :, 0:width] - log_top
    copies[2].start()
    for c in range(SEQ):
        at = c * WIDE
        low = logits[c, :, 512:768] - log_bottom
        lower_v[:, at : at + 256] = low[0:4]
        rest = min(256, VOCAB_LOCAL - at - 256)
        lower_v[:, at + 256 : at + 256 + rest] = pltpu.roll(low, 4, 0)[0:4, 0:rest]
    copies[3].start()
    for copy in copies:
        copy.wait()


def solution(mesh):
    heads_size = mesh.shape["heads"]

    def body(hidden, lengths, drafts, gain, wq, wl, cache, ku, vu, wo, fgain, wv):
        hbm = pl.BlockSpec(memory_space=pltpu.HBM)
        vmem = pl.BlockSpec(memory_space=pltpu.VMEM)
        width = GROUP_HEADS * HEAD_DIM
        results = pl.pallas_call(
            functools.partial(kernel, heads_size),
            name="decode_step",
            out_shape=(
                jax.ShapeDtypeStruct((ROWS, RANK), bf16),
                jax.ShapeDtypeStruct((SEQ, 8, 768), f32),
                jax.ShapeDtypeStruct((8, 128), f32),
                jax.ShapeDtypeStruct((1, 128), f32),
            ),
            in_specs=[hbm] * 12,
            out_specs=(vmem,) * 4,
            scratch_shapes=[
                pltpu.VMEM((ROWS, RANK), bf16),
                pltpu.SMEM((ROWS,), jnp.int32),
                pltpu.SMEM((ROWS,), jnp.int32),
                pltpu.VMEM((RANK,), f32),
                pltpu.VMEM((RANK, width), bf16),
                pltpu.VMEM((RANK, 2 * RANK), bf16),
                pltpu.VMEM((ROWS, SPAN, 2 * RANK), bf16),
                pltpu.VMEM((RANK, width), bf16),
                pltpu.VMEM((384, width), bf16),
                pltpu.VMEM((RANK, width), bf16),
                pltpu.VMEM((RANK,), f32),
                pltpu.VMEM((RANK, VOCAB_LOCAL), bf16),
                pltpu.VMEM((16, RANK), f32),
                pltpu.VMEM((256, 128), f32),
                pltpu.VMEM((256, 128), f32),
                pltpu.VMEM((256, 128), f32),
                pltpu.VMEM((3, 256, 128), f32),
                pltpu.VMEM((3, 256, 128), f32),
                pltpu.VMEM((160, 128), f32),
                pltpu.VMEM((256, 128), f32),
                pltpu.VMEM((160, 128), f32),
                pltpu.VMEM((160, 128), f32),
                pltpu.VMEM((8, 512), f32),
                pltpu.VMEM((heads_size, 8, 512), f32),
                pltpu.VMEM((1, 128), f32),
                pltpu.VMEM((SEQ, 1, 128), f32),
                pltpu.VMEM((SEQ, 8, 768), f32),
                pltpu.VMEM((SEQ, 8, 768), f32),
                pltpu.VMEM((8, 8, 768), f32),
                pltpu.VMEM((1, 128), f32),
                pltpu.VMEM((heads_size * SEQ, 1, 128), f32),
                pltpu.SemaphoreType.DMA((12,)),
                pltpu.SemaphoreType.DMA((9,)),
                pltpu.SemaphoreType.DMA((9,)),
                pltpu.SemaphoreType.DMA((heads_size,)),
                pltpu.SemaphoreType.DMA((heads_size,)),
                pltpu.SemaphoreType.REGULAR,
                pltpu.SemaphoreType.DMA((8,)),
                pltpu.SemaphoreType.DMA((8,)),
            ],
            compiler_params=pltpu.CompilerParams(
                collective_id=0, has_side_effects=True, vmem_limit_bytes=48 * 1024 * 1024
            ),
        )(*(pltpu.with_memory_space_constraint(x, pltpu.HBM) for x in (
            hidden, lengths, drafts, gain, wq, wl.reshape(RANK, 2 * RANK),
            cache.reshape(ROWS, SPAN, 2 * RANK), ku.reshape(RANK, width), vu.reshape(RANK, width),
            wo.T, fgain, wv,
        )))
        return pl.pallas_call(
            closing_kernel,
            name="outputs",
            out_shape=(
                jax.ShapeDtypeStruct((ROWS, RANK), bf16),
                jax.ShapeDtypeStruct((ROWS, VOCAB_LOCAL), f32),
                jax.ShapeDtypeStruct((ROWS,), f32),
            ),
            in_specs=[vmem] * 4,
            out_specs=(hbm,) * 3,
            scratch_shapes=[
                pltpu.VMEM((8, VOCAB_LOCAL), f32),
                pltpu.VMEM((4, VOCAB_LOCAL), f32),
                pltpu.VMEM((ROWS,), f32),
                pltpu.SemaphoreType.DMA((4,)),
            ],
            compiler_params=pltpu.CompilerParams(vmem_limit_bytes=4 * 1024 * 1024),
        )(*results)

    return jax.shard_map(
        body,
        mesh=mesh,
        in_specs=(
            P("batch", "seq"), P("batch"), P("batch"), P("seq"), P("seq", "heads"),
            P("seq", "heads", None), P("batch", "heads", "seq", None), P("heads", None, None),
            P("heads", None, None), P("heads", "seq"), P("seq"), P("seq", "heads"),
        ),
        out_specs=(P("batch", "seq"), P("batch", "heads"), P("batch")),
        check_vma=False,
    )
```
